512 devices in a mesh: seq: 64 (over y, x, core), chan: 8 (over z).
Axes of the slice: x: 4, y: 8, z: 8, core: 2. Of those that a mesh axis runs over, the one named last changes fastest.
Arguments:
- x_in: bfloat16 [131072, 2048], P('seq', 'chan'), may hold values from -6 to 6
- gate_in: bfloat16 [131072, 2048], P('seq', 'chan'), may hold values from -70 to 70
- b_in: bfloat16 [131072, 64], P('seq'), may hold values from -0.75 to 0.75
- c_in: bfloat16 [131072, 64], P('seq'), may hold values from -6 to 6
- step_size: float32 [32, 131072], P('chan', 'seq'), may hold values from 0 to 1, as said below
- log_keep: float32 [32, 131072], P('chan', 'seq'), may hold values from -2 to 0
- skip_gain: float32 [32], P('chan'), may hold values from 0.5 to 1.5
- norm_gain: float32 [2048], P('chan'), may hold values from 0.25 to 1.75
Outputs:
- mixed: bfloat16 [131072, 2048], P('seq', 'chan')
The draws below stay inside these ranges and needn't reach their ends.
Inputs may be any that keep to these rules, and one draw needn't show every extreme that they name: `step_size`: positive.
All inputs are finite; a program needn't handle non-finite values.
Results may differ from the reference program's by a relative error of at most 0.005.
Values sent between devices are 32-bit elements; how exact they have to be, the bound alone decides.
A program may use at most 64 MiB of HBM per device.

```python
import math
import jax
import jax.numpy as jnp
from jax import lax

CH = 2048
HEADDIM = 64
STATE = 64
BLOCK = 256
TOK_DEV = 2048
HEADS = 32
SEQUENCE_TOKENS = 131072


def decay_pieces(key):
    random_subkeys = jax.random.split(jax.random.fold_in(key, 17), 7)
    ranking = jax.random.permutation(random_subkeys[0], HEADS)
    slow_count = max(HEADS // 2, 1)
    is_slow = ranking < slow_count
    slow_rate = jnp.exp(jax.random.uniform(random_subkeys[1], (HEADS,), jnp.float32, math.log(0.2), math.log(0.5))) / SEQUENCE_TOKENS
    fast_rate = jnp.exp(jax.random.uniform(random_subkeys[2], (HEADS,), jnp.float32, math.log(0.02), math.log(0.05)))
    head_decay_rate = jnp.where(is_slow, slow_rate, fast_rate)
    token_multiplier = jnp.exp(jax.random.uniform(random_subkeys[3], (HEADS, SEQUENCE_TOKENS), jnp.float32, math.log(0.5), math.log(2.0)))
    device_multiplier = jnp.exp(jax.random.uniform(random_subkeys[4], (HEADS, SEQUENCE_TOKENS // TOK_DEV), jnp.float32, math.log(0.5), math.log(2.0)))
    device_multiplier = jnp.repeat(device_multiplier, TOK_DEV, axis=1)
    spike_position = jax.random.randint(random_subkeys[5], (2,), 0, SEQUENCE_TOKENS)
    spike_fraction = jax.random.uniform(random_subkeys[6], (2,), jnp.float32, 0.2, 0.5)
    token_positions = jnp.arange(SEQUENCE_TOKENS, dtype=jnp.int32)
    spike_amount = jnp.sum(jnp.where(token_positions[None, :] == spike_position[:, None], jnp.log(1.0 - spike_fraction)[:, None], 0.0), axis=0)
    return (head_decay_rate, head_decay_rate[:, None] * token_multiplier * device_multiplier, spike_amount)


def draw_log_keep(key, part):
    head_decay_rate, token_level, spike_amount = decay_pieces(key)
    return (spike_amount[None, :] - token_level).astype(jnp.float32)


def draw_step_size(key, part):
    head_decay_rate, token_level, spike_amount = decay_pieces(key)
    factor = jnp.exp(jax.random.uniform(jax.random.fold_in(key, 29), (HEADS, SEQUENCE_TOKENS), jnp.float32, math.log(0.5), math.log(2.0)))
    return (jnp.sqrt(2.0 * head_decay_rate)[:, None] * factor).astype(jnp.float32)


def draw_gate_in(key, part):
    random_subkeys = jax.random.split(jax.random.fold_in(key, 5), 2)
    column = jnp.arange(CH, dtype=jnp.float32) / max(CH - 1, 1)
    col_scale = jnp.sqrt(3.0) ** column * jnp.exp(jax.random.uniform(random_subkeys[0], (CH,), jnp.float32, 0.0, math.log(10.0)))
    noise_base = jnp.clip(jax.random.normal(random_subkeys[1], (SEQUENCE_TOKENS, CH), jnp.float32), -4.0, 4.0)
    return (noise_base * col_scale[None, :]).astype(jnp.bfloat16)


def steps_of(own_key, extent, shards, least, top_value):
    gain = 1.0
    for position, blocks in shards:
        steps = jax.random.uniform(jax.random.fold_in(jax.random.fold_in(own_key, 6), position), (blocks,), jnp.float32, least / len(shards), top_value / len(shards))
        gain = gain * jnp.repeat(jnp.exp(steps), extent[position] // blocks).reshape((-1,) + (1,) * (len(extent) - 1 - position))
    return gain


def noise(rng, dims, deviation, limit, cuts=(), kind=jnp.bfloat16):
    result = jax.random.normal(rng, dims, jnp.float32) * deviation
    if len(cuts) > 0:
        result = steps_of(rng, dims, cuts, -0.22, 0.18) * result
    return jnp.clip(result, min=-limit, max=limit).astype(kind)


def setup_inputs(seed: int = 0) -> dict:
    seeds = jax.random.split(jax.random.key(seed), 9)
    return {
        "x_in": noise(seeds[0], (SEQUENCE_TOKENS, CH), 1.0, 6.0, ((0, 64), (1, 8))),
        "gate_in": draw_gate_in(jax.random.fold_in(seeds[8], 71), 0),
        "b_in": noise(seeds[2], (SEQUENCE_TOKENS, STATE), STATE ** -0.5, 0.75, ((0, 64),)),
        "c_in": noise(seeds[3], (SEQUENCE_TOKENS, STATE), 1.0, 6.0, ((0, 64),)),
        "step_size": draw_step_size(jax.random.fold_in(seeds[8], 71), 0),
        "log_keep": draw_log_keep(jax.random.fold_in(seeds[8], 71), 0),
        "skip_gain": jnp.clip(0.5 + 1.0 * jax.random.uniform(seeds[6], (HEADS,), jnp.float32) ** steps_of(seeds[6], (HEADS,), ((0, 8),), -0.2, 0.2), 0.5, 1.5),
        "norm_gain": jnp.clip(1.0 + 0.15 * jax.random.normal(seeds[7], (CH,), jnp.float32), 0.25, 1.75),
    }


def reference(x_in, gate_in, b_in, c_in, step_size, log_keep, skip_gain, norm_gain):
    block_count = SEQUENCE_TOKENS // BLOCK
    x_blocks = x_in.reshape(block_count, BLOCK, HEADS, HEADDIM)
    b_blocks = b_in.reshape(block_count, BLOCK, STATE)
    c_blocks = c_in.reshape(block_count, BLOCK, STATE)
    keep_blocks = log_keep.reshape(HEADS, block_count, BLOCK).transpose(1, 0, 2)
    step_blocks = step_size.reshape(HEADS, block_count, BLOCK).transpose(1, 0, 2)
    row_index = lax.broadcasted_iota(jnp.int32, (BLOCK, BLOCK), 0)
    col_index = lax.broadcasted_iota(jnp.int32, (BLOCK, BLOCK), 1)
    causal = row_index >= col_index

    def advance(state_now, block_input):
        x_block, b_block, c_block, keep_block, step_block = block_input
        cum_keep = jnp.cumsum(keep_block, axis=1)
        block_total = cum_keep[:, -1]
        scores = jnp.dot(c_block, b_block.T, preferred_element_type=jnp.float32)
        log_gaps = cum_keep[:, :, None] - cum_keep[:, None, :]
        decays = jnp.where(causal[None], jnp.exp(jnp.where(causal[None], log_gaps, 0.0)), 0.0)
        weights = (scores[None] * decays * step_block[:, None, :]).astype(jnp.bfloat16)
        x_float = x_block.astype(jnp.float32)
        output = jnp.einsum('hts,shp->thp', weights.astype(jnp.float32), x_float)
        projected = jnp.einsum('tn,hpn->thp', c_block.astype(jnp.float32), state_now, precision=lax.Precision.HIGHEST)
        output = output + jnp.exp(cum_keep).T[:, :, None] * projected
        decayed_b = ((jnp.exp(block_total[:, None] - cum_keep) * step_block)[:, :, None] * b_block.astype(jnp.float32)[None]).astype(jnp.bfloat16)
        block_state = jnp.einsum('shp,hsn->hpn', x_float, decayed_b.astype(jnp.float32))
        next_state = jnp.exp(block_total)[:, None, None] * state_now + block_state
        return (next_state, output)
    initial = jnp.zeros((HEADS, HEADDIM, STATE), jnp.float32)
    _, outputs = lax.scan(advance, initial, (x_blocks, b_blocks, c_blocks, keep_blocks, step_blocks))
    recurrent = outputs + skip_gain[None, None, :, None] * x_blocks.astype(jnp.float32)
    recurrent = recurrent.reshape(SEQUENCE_TOKENS, CH)
    gated_out = recurrent * jax.nn.silu(gate_in.astype(jnp.float32))
    mean_square = lax.optimization_barrier(jnp.mean(gated_out * gated_out, axis=1))
    return (gated_out * lax.rsqrt(mean_square + 1e-05)[:, None] * norm_gain[None, :]).astype(jnp.bfloat16)
```

```python
import functools

import jax
import jax.numpy as jnp
from jax import lax
from jax.experimental import pallas as pl
from jax.experimental.pallas import tpu as pltpu
from jax.sharding import PartitionSpec as P

BLOCK = 256
LANES = 128
EPSILON = 1e-05
GROUP = 8
MESH = pl.DeviceIdType.MESH
F32 = jnp.float32
BF16 = jnp.bfloat16


def split2(v):
    high = v.astype(BF16)
    return high, (v - high.astype(F32)).astype(BF16)


def dot(a, b, contract=((1,), (0,))):
    return lax.dot_general(a, b, (contract, ((), ())), preferred_element_type=F32)


def layer(
    group, rows_y, nchan,
    x_hbm, gate_hbm, b_hbm, c_hbm, step_hbm, keep_hbm, skip_hbm, gain_hbm,
    out_hbm,
    x_s, gate_s, b_s, c_s, step_s, keep_s, skip_s, gain_s,
    keep8, step8, cum8, c2_s,
    totals, device_total, block_state, starts, prefix_s,
    end_s, gather1, totals1, group_prefix, group_total_state, group_total,
    gather2, totals2, entering_s, back_s, gather3,
    base_s, slope_s, squares_s, gather_sq, out_s,
    load_sem, skip_sem, store_sem,
    sa_send, sa_recv, sb_send, sb_recv, sc_send, sc_recv,
    sd_send, sd_recv, se_send, se_recv, sf_send, sf_recv,
):
    tokens, channels = x_s.shape
    nstate = b_s.shape[0]
    heads = keep_s.shape[0]
    width = channels // heads
    blocks = tokens // BLOCK
    tiles = channels // LANES
    per_tile = heads // tiles
    piece = nstate // group

    me = lax.axis_index("seq")
    me_z = lax.axis_index("chan")
    me_y = me // group
    me_j = me % group

    loads = [
        pltpu.make_async_copy(src, dst, load_sem.at[i])
        for i, (src, dst) in enumerate(
            (
                (keep_hbm, keep_s), (step_hbm, step_s), (b_hbm, b_s), (x_hbm, x_s),
                (c_hbm, c_s), (gate_hbm, gate_s), (gain_hbm, gain_s),
            )
        )
    ]
    loads.append(pltpu.make_async_copy(skip_hbm, skip_s, skip_sem))
    for copy in loads:
        copy.start()

    def in_group(i):
        return (me_j + i) % group

    def at_group(j):
        return (me_y * group + j, me_z)

    def at_y(y):
        return (y * group + me_j, me_z)

    barrier = pltpu.get_barrier_semaphore()
    for i in range(1, group):
        pl.semaphore_signal(barrier, inc=1, device_id=at_group(in_group(i)), device_id_type=MESH)
    for i in range(1, rows_y):
        pl.semaphore_signal(
            barrier, inc=1, device_id=at_y((me_y + i) % rows_y), device_id_type=MESH
        )
    for i in range(1, nchan):
        pl.semaphore_signal(
            barrier, inc=1, device_id=(me, (me_z + i) % nchan), device_id_type=MESH
        )

    lane = lax.broadcasted_iota(jnp.int32, (8, channels), 1)
    row8 = lax.broadcasted_iota(jnp.int32, (8, channels), 0)
    own_head = (lane // width) == row8
    half = lax.broadcasted_iota(jnp.int32, (1, LANES), 1) < width
    upper = (
        lax.broadcasted_iota(jnp.int32, (BLOCK, BLOCK), 0)
        <= lax.broadcasted_iota(jnp.int32, (BLOCK, BLOCK), 1)
    )
    upper = jnp.where(upper, 1.0, 0.0).astype(BF16)

    loads[0].wait()
    loads[1].wait()
    keep8[...] = jnp.zeros_like(keep8)
    step8[...] = jnp.zeros_like(step8)
    for k in range(blocks):
        keep8[8 * k : 8 * k + heads, :] = keep_s[:, BLOCK * k : BLOCK * (k + 1)]
        step8[8 * k : 8 * k + heads, :] = step_s[:, BLOCK * k : BLOCK * (k + 1)]
    keep = keep8[...]
    k_high = keep.astype(BF16)
    rest = keep - k_high.astype(F32)
    k_mid, k_low = split2(rest)
    cum8[...] = dot(k_high, upper) + (dot(k_mid, upper) + dot(k_low, upper))

    for k in range(blocks):
        last = cum8[8 * k : 8 * k + 8, BLOCK - 1 : BLOCK]
        spread = jnp.where(own_head, jnp.broadcast_to(last, (8, channels)), 0.0)
        totals[k : k + 1, :] = jnp.sum(spread, axis=0, keepdims=True)
    device_total[...] = jnp.broadcast_to(
        jnp.sum(totals[...], axis=0, keepdims=True), device_total.shape
    )

    pl.semaphore_wait(barrier, group + rows_y + nchan - 3)

    def copy_a(i):
        return pltpu.make_async_remote_copy(
            device_total, totals1.at[me_j], sa_send.at[i], sa_recv.at[me_j],
            device_id=at_group(in_group(i)), device_id_type=MESH,
        )

    for i in range(1, group):
        copy_a(i).start()

    loads[2].wait()
    loads[3].wait()
    for k in range(blocks):
        slab = cum8[8 * k : 8 * k + 8, :]
        coef = jnp.exp(slab[:, BLOCK - 1 : BLOCK] - slab) * step8[8 * k : 8 * k + 8, :]
        bt = b_s[:, BLOCK * k : BLOCK * (k + 1)].astype(F32)
        for t in range(tiles):
            left = jnp.concatenate(
                [(bt * coef[h : h + 1, :]).astype(BF16) for h in (2 * t, 2 * t + 1)], axis=0
            )
            both = dot(left, x_s[BLOCK * k : BLOCK * (k + 1), LANES * t : LANES * (t + 1)])
            block_state[k, :, LANES * t : LANES * (t + 1)] = jnp.where(
                half, both[:nstate], both[nstate:]
            )
    running = jnp.zeros((nstate, channels), F32)
    for k in range(blocks):
        starts[k] = running
        running = jnp.exp(totals[k : k + 1, :]) * running + block_state[k]
    for p in range(group):
        end_s[p] = running[piece * p : piece * (p + 1), :]

    def copy_b(i):
        p = in_group(i)
        return pltpu.make_async_remote_copy(
            end_s.at[p], gather1.at[me_j], sb_send.at[i], sb_recv.at[me_j],
            device_id=at_group(p), device_id_type=MESH,
        )

    for i in range(1, group):
        copy_b(i).start()
    gather1[me_j] = end_s[me_j]
    totals1[me_j] = device_total[...]

    before = jnp.zeros((1, channels), F32)
    for k in range(blocks):
        prefix_s[k : k + 1, :] = before
        before = before + totals[k : k + 1, :]

    for i in range(4, len(loads)):
        loads[i].wait()
    head_of = lax.broadcasted_iota(jnp.int32, (1, channels), 1) // width
    skip_row = jnp.zeros((1, channels), F32)
    for h in range(heads):
        skip_row = jnp.where(head_of == h, skip_s[0, h], skip_row)
    diagonal = (
        lax.broadcasted_iota(jnp.int32, (LANES, LANES), 0)
        >= lax.broadcasted_iota(jnp.int32, (LANES, LANES), 1)
    )

    def inside(k, carry):
        rows = pl.ds(pl.multiple_of(k * BLOCK, BLOCK), BLOCK)
        slab_at = pl.ds(pl.multiple_of(k * 8, 8), 8)
        slab = cum8[slab_at, :]
        steps = step8[slab_at, :]
        columns = jnp.transpose(slab)
        c_block = c_s[:, rows]
        c_pair = jnp.transpose(jnp.concatenate([c_block, c_block], axis=0))
        c2_s[rows, :] = c_pair
        scores = dot(c_pair[:, :nstate], b_s[:, rows])
        for t in range(tiles):
            lanes = slice(LANES * t, LANES * (t + 1))
            weights, spreads = [], []
            for h in (2 * t, 2 * t + 1):
                column = jnp.broadcast_to(columns[:, h : h + 1], (BLOCK, LANES))
                spreads.append(column)

                def weight(r, s):
                    rr, ss = slice(LANES * r, LANES * (r + 1)), slice(LANES * s, LANES * (s + 1))
                    w = (
                        scores[rr, ss]
                        * jnp.exp(column[rr, :] - slab[h : h + 1, ss])
                        * steps[h : h + 1, ss]
                    )
                    return (jnp.where(diagonal, w, 0.0) if r == s else w).astype(BF16)

                top = jnp.concatenate([weight(0, 0), jnp.zeros((LANES, LANES), BF16)], axis=1)
                bottom = jnp.concatenate([weight(1, 0), weight(1, 1)], axis=1)
                weights += [top, bottom]
            x_tile = x_s[rows, lanes]
            both = dot(jnp.concatenate(weights, axis=0), x_tile)
            value = jnp.where(half, both[:BLOCK], both[BLOCK:])
            value = value + skip_row[:, lanes] * x_tile.astype(F32)
            gate = gate_s[rows, lanes].astype(F32)
            gate = gate / (1.0 + jnp.exp(-gate))
            base_s[rows, lanes] = value * gate
            slope_s[rows, lanes] = jnp.exp(jnp.where(half, spreads[0], spreads[1])) * gate
        return carry

    cuts = (0, (blocks * 3) // 8, (blocks * 6) // 8, blocks)
    lax.fori_loop(cuts[0], cuts[1], inside, 0)

    for m in range(group):

        @pl.when(m != me_j)
        def _():
            pltpu.make_async_remote_copy(
                device_total, totals1.at[m], sa_send.at[0], sa_recv.at[m],
                device_id=at_group(m), device_id_type=MESH,
            ).wait_recv()

    total = totals1[0]
    for m in range(1, group):
        total = total + totals1[m]
    group_total[...] = total

    def copy_c(i):
        return pltpu.make_async_remote_copy(
            group_total, totals2.at[me_y], sc_send.at[i], sc_recv.at[me_y],
            device_id=at_y(me_y + i), device_id_type=MESH,
        )

    def copy_d(i):
        return pltpu.make_async_remote_copy(
            group_total_state, gather2.at[me_y], sd_send.at[i], sd_recv.at[me_y],
            device_id=at_y(me_y + i), device_id_type=MESH,
        )

    for i in range(1, rows_y):

        @pl.when(me_y + i < rows_y)
        def _():
            copy_c(i).start()

    for m in range(group):

        @pl.when(m != me_j)
        def _():
            pltpu.make_async_remote_copy(
                end_s.at[m], gather1.at[m], sb_send.at[0], sb_recv.at[m],
                device_id=at_group(m), device_id_type=MESH,
            ).wait_recv()

    state = jnp.zeros((piece, channels), F32)
    for m in range(group):
        group_prefix[m] = state
        state = jnp.exp(totals1[m, 0:1, :]) * state + gather1[m]
    group_total_state[...] = state
    for i in range(1, rows_y):

        @pl.when(me_y + i < rows_y)
        def _():
            copy_d(i).start()

    lax.fori_loop(cuts[1], cuts[2], inside, 0)

    entering_s[...] = jnp.zeros_like(entering_s)
    for y in range(rows_y - 1):

        @pl.when(y < me_y)
        def _():
            pltpu.make_async_remote_copy(
                group_total, totals2.at[y], sc_send.at[0], sc_recv.at[y],
                device_id=at_y(y), device_id_type=MESH,
            ).wait_recv()
            pltpu.make_async_remote_copy(
                group_total_state, gather2.at[y], sd_send.at[0], sd_recv.at[y],
                device_id=at_y(y), device_id_type=MESH,
            ).wait_recv()
            entering_s[...] = jnp.exp(totals2[y, 0:1, :]) * entering_s[...] + gather2[y]

    entering = entering_s[...]
    ahead = jnp.zeros((1, channels), F32)
    for m in range(group):
        back_s[m] = jnp.exp(ahead) * entering + group_prefix[m]
        ahead = ahead + totals1[m, 0:1, :]

    def copy_e(i):
        p = in_group(i)
        return pltpu.make_async_remote_copy(
            back_s.at[p], gather3.at[me_j], se_send.at[i], se_recv.at[me_j],
            device_id=at_group(p), device_id_type=MESH,
        )

    for i in range(1, group):
        copy_e(i).start()
    gather3[me_j] = back_s[me_j]

    lax.fori_loop(cuts[2], cuts[3], inside, 0)

    for m in range(group):

        @pl.when(m != me_j)
        def _():
            pltpu.make_async_remote_copy(
                back_s.at[m], gather3.at[m], se_send.at[0], se_recv.at[m],
                device_id=at_group(m), device_id_type=MESH,
            ).wait_recv()

    incoming = jnp.concatenate([gather3[p] for p in range(group)], axis=0)
    ones = jnp.ones((8, BLOCK), BF16)
    for k in range(blocks):
        rows = slice(BLOCK * k, BLOCK * (k + 1))
        at_start = starts[k] + jnp.exp(prefix_s[k : k + 1, :]) * incoming
        high, low = split2(at_start)
        read = dot(c2_s[rows, :], jnp.concatenate([high, low], axis=0))
        gated = base_s[rows, :] + slope_s[rows, :] * read
        base_s[rows, :] = gated
        square = gated * gated
        partial = square[:, :LANES]
        for t in range(1, tiles):
            partial = partial + square[:, LANES * t : LANES * (t + 1)]
        high, low = split2(partial)
        row = dot(ones, jnp.concatenate([high, low], axis=1), ((1,), (1,)))
        squares_s[k : k + 1, :] = row[0:1, :]

    def copy_f(i):
        return pltpu.make_async_remote_copy(
            squares_s, gather_sq.at[me_z], sf_send.at[i], sf_recv.at[me_z],
            device_id=(me, (me_z + i) % nchan), device_id_type=MESH,
        )

    for i in range(1, nchan):
        copy_f(i).start()
    gather_sq[me_z] = squares_s[...]
    for z in range(nchan):

        @pl.when(z != me_z)
        def _():
            pltpu.make_async_remote_copy(
                squares_s, gather_sq.at[z], sf_send.at[0], sf_recv.at[z],
                device_id=(me, z), device_id_type=MESH,
            ).wait_recv()

    total = gather_sq[0]
    for z in range(1, nchan):
        total = total + gather_sq[z]
    factor = jnp.transpose(lax.rsqrt(total / (channels * nchan) + EPSILON))
    gain = gain_s[...]
    stores = []
    for k in range(blocks):
        rows = slice(BLOCK * k, BLOCK * (k + 1))
        scale = jnp.broadcast_to(factor[:, k : k + 1], (BLOCK, LANES))
        for t in range(tiles):
            lanes = slice(LANES * t, LANES * (t + 1))
            out_s[rows, lanes] = (base_s[rows, lanes] * scale * gain[:, lanes]).astype(BF16)
        store = pltpu.make_async_copy(out_s.at[rows, :], out_hbm.at[rows, :], store_sem.at[k])
        store.start()
        stores.append(store)

    for i in range(1, group):
        copy_a(i).wait_send()
        copy_b(i).wait_send()
        copy_e(i).wait_send()
    for i in range(1, rows_y):

        @pl.when(me_y + i < rows_y)
        def _():
            copy_c(i).wait_send()
            copy_d(i).wait_send()

    for i in range(1, nchan):
        copy_f(i).wait_send()
    for store in stores:
        store.wait()


def per_device(group, rows_y, nchan, x, gate, b, c, step, keep, skip, gain):
    tokens, channels = x.shape
    nstate = b.shape[1]
    heads = step.shape[0]
    blocks = tokens // BLOCK
    piece = nstate // group
    vmem = pltpu.VMEM
    dma = pltpu.SemaphoreType.DMA
    anywhere = pl.BlockSpec(memory_space=pl.ANY)
    scratch = [
        vmem((tokens, channels), BF16), vmem((tokens, channels), BF16),
        vmem((nstate, tokens), BF16), vmem((nstate, tokens), BF16),
        vmem((heads, tokens), F32), vmem((heads, tokens), F32),
        pltpu.SMEM((1, heads), F32), vmem((1, channels), F32),
        vmem((8 * blocks, BLOCK), F32), vmem((8 * blocks, BLOCK), F32),
        vmem((8 * blocks, BLOCK), F32),
        vmem((tokens, 2 * nstate), BF16),
        vmem((blocks, channels), F32), vmem((8, channels), F32),
        vmem((blocks, nstate, channels), F32), vmem((blocks, nstate, channels), F32),
        vmem((blocks, channels), F32),
        vmem((group, piece, channels), F32), vmem((group, piece, channels), F32),
        vmem((group, 8, channels), F32), vmem((group, piece, channels), F32),
        vmem((piece, channels), F32), vmem((8, channels), F32),
        vmem((rows_y, piece, channels), F32), vmem((rows_y, 8, channels), F32),
        vmem((piece, channels), F32),
        vmem((group, piece, channels), F32), vmem((group, piece, channels), F32),
        vmem((tokens, channels), F32), vmem((tokens, channels), F32),
        vmem((blocks, BLOCK), F32), vmem((nchan, blocks, BLOCK), F32),
        vmem((tokens, channels), BF16),
        dma((7,)), dma, dma((blocks,)),
        dma((group,)), dma((group,)), dma((group,)), dma((group,)),
        dma((rows_y,)), dma((rows_y,)), dma((rows_y,)), dma((rows_y,)),
        dma((group,)), dma((group,)), dma((nchan,)), dma((nchan,)),
    ]
    return pl.pallas_call(
        functools.partial(layer, group, rows_y, nchan),
        out_shape=jax.ShapeDtypeStruct((tokens, channels), BF16),
        in_specs=[anywhere] * 8,
        out_specs=anywhere,
        scratch_shapes=scratch,
        compiler_params=pltpu.CompilerParams(collective_id=0, has_side_effects=True),
    )(x, gate, b.T, c.T, step, keep, skip.reshape(1, heads), gain.reshape(1, channels))


def build(mesh, group):
    rows_y = mesh.shape["seq"] // group
    placed = (
        P("seq", "chan"), P("seq", "chan"), P("seq", None), P("seq", None),
        P("chan", "seq"), P("chan", "seq"), P("chan"), P("chan"),
    )
    return jax.shard_map(
        functools.partial(per_device, group, rows_y, mesh.shape["chan"]),
        mesh=mesh, in_specs=placed, out_specs=P("seq", "chan"), check_vma=False,
    )


def solution(mesh):
    return build(mesh, GROUP)
```

```python
import functools

import jax
import jax.numpy as jnp
from jax import lax
from jax.experimental import pallas as pl
from jax.experimental.pallas import tpu as pltpu
from jax.sharding import PartitionSpec as P

BLOCK = 256
LANES = 128
EPSILON = 1e-05
GROUP = 8
MESH = pl.DeviceIdType.MESH
F32 = jnp.float32
BF16 = jnp.bfloat16


def split2(v):
    high = v.astype(BF16)
    return high, (v - high.astype(F32)).astype(BF16)


def dot(a, b, contract=((1,), (0,))):
    return lax.dot_general(a, b, (contract, ((), ())), preferred_element_type=F32)


def layer(
    group, rows_y, nchan,
    x_hbm, gate_hbm, b_hbm, c_hbm, step_hbm, keep_hbm, skip_hbm, gain_hbm,
    out_ref,
    x_s, gate_s, b_s, c_s, step_s, keep_s, skip_s, gain_s,
    keep8, step8, cum8, c2_s,
    totals, device_total, block_state, starts, prefix_s,
    end_s, gather1, totals1, group_prefix, group_total_state, group_total,
    gather2, totals2, entering_s, back_s, gather3,
    base_s, slope_s, squares_s, gather_sq,
    load_sem, skip_sem, y_in, z_in,
    sa_send, sa_recv, sb_send, sb_recv, sc_send, sc_recv,
    sd_send, sd_recv, se_send, se_recv, sf_send, sf_recv,
):
    tokens, channels = x_s.shape
    nstate = b_s.shape[0]
    heads = keep_s.shape[0]
    width = channels // heads
    blocks = tokens // BLOCK
    tiles = channels // LANES
    per_tile = heads // tiles
    piece = 2 * nstate // group

    me = lax.axis_index("seq")
    me_z = lax.axis_index("chan")
    me_y = me // group
    me_j = me % group
    is_owner = me_j % 2 == 1
    me_q = me_j // 2

    def owner(q):
        return 2 * q + 1

    def at_group(j):
        return (me_y * group + j, me_z)

    def at_y(y):
        return (y * group + me_j, me_z)

    def rank(y):
        return jnp.minimum(y, rows_y - y) * rows_y + y

    barrier = pltpu.get_barrier_semaphore()

    def greet(device):
        pl.semaphore_signal(barrier, inc=1, device_id=device, device_id_type=MESH)

    def report(semaphore, device):
        pl.semaphore_signal(semaphore, inc=1, device_id=device, device_id_type=MESH)

    for j in range(group):

        @pl.when((j != me_j) & (is_owner | (j % 2 == 1)))
        def _():
            greet(at_group(j))

    for y in range(rows_y):

        @pl.when(is_owner & (rank(me_y) < rank(y)))
        def _():
            greet(at_y(y))

    for z in range(nchan):

        @pl.when(me_z < z)
        def _():
            greet((me, z))

    loads = [
        pltpu.make_async_copy(src, dst, load_sem.at[i])
        for i, (src, dst) in enumerate(
            (
                (keep_hbm, keep_s), (step_hbm, step_s), (b_hbm, b_s), (x_hbm, x_s),
                (c_hbm, c_s), (gate_hbm, gate_s), (gain_hbm, gain_s),
            )
        )
    ]
    loads.append(pltpu.make_async_copy(skip_hbm, skip_s, skip_sem))
    for copy in loads:
        copy.start()

    lane = lax.broadcasted_iota(jnp.int32, (8, channels), 1)
    row8 = lax.broadcasted_iota(jnp.int32, (8, channels), 0)
    own_head = (lane // width) == row8
    half = lax.broadcasted_iota(jnp.int32, (1, LANES), 1) < width
    upper = (
        lax.broadcasted_iota(jnp.int32, (BLOCK, BLOCK), 0)
        <= lax.broadcasted_iota(jnp.int32, (BLOCK, BLOCK), 1)
    )
    upper = jnp.where(upper, 1.0, 0.0).astype(BF16)

    loads[0].wait()
    loads[1].wait()
    keep8[...] = jnp.zeros_like(keep8)
    step8[...] = jnp.zeros_like(step8)
    for k in range(blocks):
        keep8[8 * k : 8 * k + heads, :] = keep_s[:, BLOCK * k : BLOCK * (k + 1)]
        step8[8 * k : 8 * k + heads, :] = step_s[:, BLOCK * k : BLOCK * (k + 1)]
    keep = keep8[...]
    k_high = keep.astype(BF16)
    rest = keep - k_high.astype(F32)
    k_mid, k_low = split2(rest)
    cum8[...] = dot(k_high, upper) + (dot(k_mid, upper) + dot(k_low, upper))

    for k in range(blocks):
        last = cum8[8 * k : 8 * k + 8, BLOCK - 1 : BLOCK]
        spread = jnp.where(own_head, jnp.broadcast_to(last, (8, channels)), 0.0)
        totals[k : k + 1, :] = jnp.sum(spread, axis=0, keepdims=True)
    device_total[...] = jnp.sum(totals[...], axis=0, keepdims=True)

    loads[2].wait()
    loads[3].wait()
    for k in range(blocks):
        slab = cum8[8 * k : 8 * k + 8, :]
        coef = jnp.exp(slab[:, BLOCK - 1 : BLOCK] - slab) * step8[8 * k : 8 * k + 8, :]
        bt = b_s[:, BLOCK * k : BLOCK * (k + 1)].astype(F32)
        for t in range(tiles):
            left = jnp.concatenate(
                [(bt * coef[h : h + 1, :]).astype(BF16) for h in (2 * t, 2 * t + 1)], axis=0
            )
            both = dot(left, x_s[BLOCK * k : BLOCK * (k + 1), LANES * t : LANES * (t + 1)])
            block_state[k, :, LANES * t : LANES * (t + 1)] = jnp.where(
                half, both[:nstate], both[nstate:]
            )
    running = jnp.zeros((nstate, channels), F32)
    for k in range(blocks):
        starts[k] = running
        running = jnp.exp(totals[k : k + 1, :]) * running + block_state[k]
    for q in range(group // 2):
        end_s[q] = running[piece * q : piece * (q + 1), :]

    greeted = me_z + jnp.where(is_owner, group - 1, group // 2)
    expected_y = 0
    for y in range(rows_y):
        greeted = greeted + jnp.where(is_owner & (rank(y) < rank(me_y)), 1, 0)
        expected_y = expected_y + jnp.where((y > me_y) & (rank(y) > rank(me_y)), 1, 0)
    pl.semaphore_wait(barrier, greeted)

    def copy_a(i):
        return pltpu.make_async_remote_copy(
            device_total, totals1.at[me_j], sa_send.at[i], sa_recv.at[me_j],
            device_id=at_group(owner((me_q + i) % (group // 2))), device_id_type=MESH,
        )

    def copy_b(i):
        q = (me_q + i) % (group // 2)
        return pltpu.make_async_remote_copy(
            end_s.at[q], gather1.at[me_j], sb_send.at[i], sb_recv.at[me_j],
            device_id=at_group(owner(q)), device_id_type=MESH,
        )

    others = [group // 4] + [i for i in range(group // 2) if i != group // 4]
    for i in others:

        @pl.when((i != 0) | jnp.logical_not(is_owner))
        def _():
            copy_a(i).start()
            copy_b(i).start()

    for z in range(nchan):

        @pl.when(z < me_z)
        def _():
            report(z_in, (me, z))

    for y in range(rows_y):

        @pl.when(is_owner & (y < me_y) & (rank(y) < rank(me_y)))
        def _():
            report(y_in, at_y(y))

    @pl.when(is_owner)
    def _():
        gather1[me_j] = end_s[me_q]
        totals1[me_j] = device_total[...]

    before = jnp.zeros((1, channels), F32)
    for k in range(blocks):
        prefix_s[k : k + 1, :] = before
        before = before + totals[k : k + 1, :]

    for i in range(4, len(loads)):
        loads[i].wait()
    head_of = lax.broadcasted_iota(jnp.int32, (1, channels), 1) // width
    skip_row = jnp.zeros((1, channels), F32)
    for h in range(heads):
        skip_row = jnp.where(head_of == h, skip_s[0, h], skip_row)
    diagonal = (
        lax.broadcasted_iota(jnp.int32, (LANES, LANES), 0)
        >= lax.broadcasted_iota(jnp.int32, (LANES, LANES), 1)
    )

    def inside(k, carry):
        rows = pl.ds(pl.multiple_of(k * BLOCK, BLOCK), BLOCK)
        slab_at = pl.ds(pl.multiple_of(k * 8, 8), 8)
        slab = cum8[slab_at, :]
        steps = step8[slab_at, :]
        columns = jnp.transpose(slab)
        c_block = c_s[:, rows]
        c_pair = jnp.transpose(jnp.concatenate([c_block, c_block], axis=0))
        c2_s[rows, :] = c_pair
        scores = dot(c_pair[:, :nstate], b_s[:, rows])
        for t in range(tiles):
            lanes = slice(LANES * t, LANES * (t + 1))
            weights, spreads = [], []
            for h in (2 * t, 2 * t + 1):
                column = jnp.broadcast_to(columns[:, h : h + 1], (BLOCK, LANES))
                spreads.append(column)

                def weight(r, s):
                    rr, ss = slice(LANES * r, LANES * (r + 1)), slice(LANES * s, LANES * (s + 1))
                    w = (
                        scores[rr, ss]
                        * jnp.exp(column[rr, :] - slab[h : h + 1, ss])
                        * steps[h : h + 1, ss]
                    )
                    return (jnp.where(diagonal, w, 0.0) if r == s else w).astype(BF16)

                top = jnp.concatenate([weight(0, 0), jnp.zeros((LANES, LANES), BF16)], axis=1)
                bottom = jnp.concatenate([weight(1, 0), weight(1, 1)], axis=1)
                weights += [top, bottom]
            x_tile = x_s[rows, lanes]
            both = dot(jnp.concatenate(weights, axis=0), x_tile)
            value = jnp.where(half, both[:BLOCK], both[BLOCK:])
            value = value + skip_row[:, lanes] * x_tile.astype(F32)
            gate = gate_s[rows, lanes].astype(F32)
            gate = gate / (1.0 + jnp.exp(-gate))
            base_s[rows, lanes] = value * gate
            slope_s[rows, lanes] = jnp.exp(jnp.where(half, spreads[0], spreads[1])) * gate
        return carry

    cuts = (0, blocks // 2, blocks)
    lax.fori_loop(cuts[0], cuts[1], inside, 0)

    def copy_c(i):
        return pltpu.make_async_remote_copy(
            group_total, totals2.at[me_y], sc_send.at[i], sc_recv.at[me_y],
            device_id=at_y(me_y + i), device_id_type=MESH,
        )

    def copy_d(i):
        return pltpu.make_async_remote_copy(
            group_total_state, gather2.at[me_y], sd_send.at[i], sd_recv.at[me_y],
            device_id=at_y(me_y + i), device_id_type=MESH,
        )

    @pl.when(is_owner)
    def _():
        @pl.when(expected_y > 0)
        def _():
            pl.semaphore_wait(y_in, expected_y)

        for m in range(group):

            @pl.when(m != me_j)
            def _():
                pltpu.make_async_remote_copy(
                    device_total, totals1.at[m], sa_send.at[0], sa_recv.at[m],
                    device_id=at_group(m), device_id_type=MESH,
                ).wait_recv()

        total = totals1[0]
        for m in range(1, group):
            total = total + totals1[m]
        group_total[...] = total
        for i in range(1, rows_y):

            @pl.when(me_y + i < rows_y)
            def _():
                copy_c(i).start()

        for m in range(group):

            @pl.when(m != me_j)
            def _():
                pltpu.make_async_remote_copy(
                    end_s.at[0], gather1.at[m], sb_send.at[0], sb_recv.at[m],
                    device_id=at_group(m), device_id_type=MESH,
                ).wait_recv()

        state = jnp.zeros((piece, channels), F32)
        for m in range(group):
            group_prefix[m] = state
            state = jnp.exp(totals1[m]) * state + gather1[m]
        group_total_state[...] = state
        for i in range(1, rows_y):

            @pl.when(me_y + i < rows_y)
            def _():
                copy_d(i).start()


    def copy_e(i):
        p = (me_j + i) % group
        return pltpu.make_async_remote_copy(
            back_s.at[p], gather3.at[me_q], se_send.at[i], se_recv.at[me_q],
            device_id=at_group(p), device_id_type=MESH,
        )

    @pl.when(is_owner)
    def _():
        entering_s[...] = jnp.zeros_like(entering_s)
        for y in range(rows_y - 1):

            @pl.when(y < me_y)
            def _():
                pltpu.make_async_remote_copy(
                    group_total, totals2.at[y], sc_send.at[0], sc_recv.at[y],
                    device_id=at_y(y), device_id_type=MESH,
                ).wait_recv()
                pltpu.make_async_remote_copy(
                    group_total_state, gather2.at[y], sd_send.at[0], sd_recv.at[y],
                    device_id=at_y(y), device_id_type=MESH,
                ).wait_recv()
                entering_s[...] = jnp.exp(totals2[y]) * entering_s[...] + gather2[y]

        entering = entering_s[...]
        ahead = jnp.zeros((1, channels), F32)
        for m in range(group):
            back_s[m] = jnp.exp(ahead) * entering + group_prefix[m]
            ahead = ahead + totals1[m]
        far = sorted(range(1, group), key=lambda i: -min((i + 1) // 2, (group - i) // 2 + 1))
        for i in far:
            copy_e(i).start()
        gather3[me_q] = back_s[me_j]

    lax.fori_loop(cuts[1], cuts[2], inside, 0)

    for q in range(group // 2):

        @pl.when(owner(q) != me_j)
        def _():
            pltpu.make_async_remote_copy(
                back_s.at[0], gather3.at[q], se_send.at[0], se_recv.at[q],
                device_id=at_group(owner(q)), device_id_type=MESH,
            ).wait_recv()

    incoming = jnp.concatenate([gather3[q] for q in range(group // 2)], axis=0)
    ones = jnp.ones((8, BLOCK), BF16)
    for k in range(blocks):
        rows = slice(BLOCK * k, BLOCK * (k + 1))
        at_start = starts[k] + jnp.exp(prefix_s[k : k + 1, :]) * incoming
        high, low = split2(at_start)
        read = dot(c2_s[rows, :], jnp.concatenate([high, low], axis=0))
        gated = base_s[rows, :] + slope_s[rows, :] * read
        base_s[rows, :] = gated
        square = gated * gated
        partial = square[:, :LANES]
        for t in range(1, tiles):
            partial = partial + square[:, LANES * t : LANES * (t + 1)]
        high, low = split2(partial)
        row = dot(ones, jnp.concatenate([high, low], axis=1), ((1,), (1,)))
        squares_s[k : k + 1, :] = row[0:1, :]

    def copy_f(z):
        return pltpu.make_async_remote_copy(
            squares_s, gather_sq.at[me_z], sf_send.at[z], sf_recv.at[me_z],
            device_id=(me, z), device_id_type=MESH,
        )

    for z in range(nchan):

        @pl.when(z < me_z)
        def _():
            copy_f(z).start()

    @pl.when(me_z < nchan - 1)
    def _():
        pl.semaphore_wait(z_in, nchan - 1 - me_z)

    for z in range(nchan):

        @pl.when(z > me_z)
        def _():
            copy_f(z).start()

    gather_sq[me_z] = squares_s[...]
    for k in range(blocks):
        rows = slice(BLOCK * k, BLOCK * (k + 1))
        base_s[rows, :] = base_s[rows, :] * gain_s[...]

    for z in range(nchan):

        @pl.when(z != me_z)
        def _():
            pltpu.make_async_remote_copy(
                squares_s, gather_sq.at[z], sf_send.at[z], sf_recv.at[z],
                device_id=(me, z), device_id_type=MESH,
            ).wait_recv()

    total = gather_sq[0]
    for z in range(1, nchan):
        total = total + gather_sq[z]
    factor = jnp.transpose(lax.rsqrt(total / (channels * nchan) + EPSILON))
    for k in range(blocks):
        rows = slice(BLOCK * k, BLOCK * (k + 1))
        scale = jnp.broadcast_to(factor[:, k : k + 1], (BLOCK, LANES))
        for t in range(tiles):
            lanes = slice(LANES * t, LANES * (t + 1))
            out_ref[rows, lanes] = (base_s[rows, lanes] * scale).astype(BF16)

    for i in range(group // 2):

        @pl.when((i != 0) | jnp.logical_not(is_owner))
        def _():
            copy_a(i).wait_send()
            copy_b(i).wait_send()

    @pl.when(is_owner)
    def _():
        for i in range(1, rows_y):

            @pl.when(me_y + i < rows_y)
            def _():
                copy_c(i).wait_send()
                copy_d(i).wait_send()

        for i in range(1, group):
            copy_e(i).wait_send()

    for z in range(nchan):

        @pl.when(z != me_z)
        def _():
            copy_f(z).wait_send()


def per_device(group, rows_y, nchan, x, gate, b, c, step, keep, skip, gain):
    tokens, channels = x.shape
    nstate = b.shape[1]
    heads = step.shape[0]
    blocks = tokens // BLOCK
    owners = group // 2
    piece = nstate // owners
    vmem = pltpu.VMEM
    dma = pltpu.SemaphoreType.DMA
    anywhere = pl.BlockSpec(memory_space=pl.ANY)
    operands = (x, gate, b.T, c.T, step, keep, skip.reshape(1, heads), gain.reshape(1, channels))
    scratch = [
        vmem((tokens, channels), BF16), vmem((tokens, channels), BF16),
        vmem((nstate, tokens), BF16), vmem((nstate, tokens), BF16),
        vmem((heads, tokens), F32), vmem((heads, tokens), F32),
        pltpu.SMEM((1, heads), F32), vmem((1, channels), F32),
        vmem((8 * blocks, BLOCK), F32), vmem((8 * blocks, BLOCK), F32),
        vmem((8 * blocks, BLOCK), F32),
        vmem((tokens, 2 * nstate), BF16),
        vmem((blocks, channels), F32), vmem((1, channels), F32),
        vmem((blocks, nstate, channels), F32), vmem((blocks, nstate, channels), F32),
        vmem((blocks, channels), F32),
        vmem((owners, piece, channels), F32), vmem((group, piece, channels), F32),
        vmem((group, 1, channels), F32), vmem((group, piece, channels), F32),
        vmem((piece, channels), F32), vmem((1, channels), F32),
        vmem((rows_y, piece, channels), F32), vmem((rows_y, 1, channels), F32),
        vmem((piece, channels), F32),
        vmem((group, piece, channels), F32), vmem((owners, piece, channels), F32),
        vmem((tokens, channels), F32), vmem((tokens, channels), F32),
        vmem((blocks, BLOCK), F32), vmem((nchan, blocks, BLOCK), F32),
        dma((7,)), dma, pltpu.SemaphoreType.REGULAR, pltpu.SemaphoreType.REGULAR,
        dma((owners,)), dma((group,)), dma((owners,)), dma((group,)),
        dma((rows_y,)), dma((rows_y,)), dma((rows_y,)), dma((rows_y,)),
        dma((group,)), dma((owners,)), dma((nchan,)), dma((nchan,)),
    ]
    return pl.pallas_call(
        functools.partial(layer, group, rows_y, nchan),
        out_shape=jax.ShapeDtypeStruct((tokens, channels), BF16),
        in_specs=[anywhere] * 8,
        out_specs=pl.BlockSpec(memory_space=pltpu.VMEM),
        scratch_shapes=scratch,
        compiler_params=pltpu.CompilerParams(
            collective_id=0, has_side_effects=True, vmem_limit_bytes=24 * 1024 * 1024
        ),
    )(*[pltpu.with_memory_space_constraint(v, pltpu.HBM) for v in operands])


def build(mesh, group):
    rows_y = mesh.shape["seq"] // group
    placed = (
        P("seq", "chan"), P("seq", "chan"), P("seq", None), P("seq", None),
        P("chan", "seq"), P("chan", "seq"), P("chan"), P("chan"),
    )
    return jax.shard_map(
        functools.partial(per_device, group, rows_y, mesh.shape["chan"]),
        mesh=mesh, in_specs=placed, out_specs=P("seq", "chan"), check_vma=False,
    )


def solution(mesh):
    return build(mesh, GROUP)
```

```python
import functools

import jax
import jax.numpy as jnp
from jax import lax
from jax.experimental import pallas as pl
from jax.experimental.pallas import tpu as pltpu
from jax.sharding import PartitionSpec as P

BLOCK = 256
LANES = 128
EPSILON = 1e-05
GROUP = 8
MESH = pl.DeviceIdType.MESH
F32 = jnp.float32
BF16 = jnp.bfloat16


def split2(v):
    high = v.astype(BF16)
    return high, (v - high.astype(F32)).astype(BF16)


def dot(a, b, contract=((1,), (0,))):
    return lax.dot_general(a, b, (contract, ((), ())), preferred_element_type=F32)


def layer(
    group, rows_y, nchan,
    x_hbm, gate_hbm, b_hbm, c_hbm, step_hbm, keep_hbm, skip_hbm, gain_hbm,
    base_s, total_ref,
    x_s, gate_s, b_s, c_s, keep_step, skip_s, gain_s,
    keep8, step8, coef8, cum8, c2_s,
    totals, device_total, block_state, starts, prefix_s,
    end_s, gather1, totals1, group_prefix, group_total_state, group_total,
    gather2, totals2, entering_s, back_s, gather3,
    slope_s, squares_s, gather_sq,
    load_sem, keep_sem, skip_sem, y_in, z_in,
    sa_send, sa_recv, sb_send, sb_recv, sc_send, sc_recv,
    sd_send, sd_recv, se_send, se_recv, sf_send, sf_recv,
):
    tokens, channels = x_s.shape
    nstate = b_s.shape[0]
    heads = keep_step.shape[1]
    width = channels // heads
    blocks = tokens // BLOCK
    tiles = channels // LANES
    per_tile = heads // tiles
    piece = 2 * nstate // group

    me = lax.axis_index("seq")
    me_z = lax.axis_index("chan")
    me_y = me // group
    me_j = me % group
    is_owner = me_j % 2 == 1
    me_q = me_j // 2

    def owner(q):
        return 2 * q + 1

    def at_group(j):
        return (me_y * group + j, me_z)

    def at_y(y):
        return (y * group + me_j, me_z)

    def arrived(ref, semaphore):
        pltpu.make_async_remote_copy(
            ref, ref, semaphore, semaphore,
            device_id=(me, (me_z + 1) % nchan), device_id_type=MESH,
        ).wait_recv()

    def sent(ref, semaphore):
        pltpu.make_async_remote_copy(
            ref, ref, semaphore, semaphore,
            device_id=(me, (me_z + 1) % nchan), device_id_type=MESH,
        ).wait_send()

    def rank(y):
        return jnp.minimum(y, rows_y - y) * rows_y + y

    first = [
        pltpu.make_async_copy(keep_hbm, keep_step.at[0], keep_sem),
        pltpu.make_async_copy(step_hbm, keep_step.at[1], keep_sem),
        pltpu.make_async_copy(b_hbm, b_s, load_sem.at[0]),
        pltpu.make_async_copy(x_hbm, x_s, load_sem.at[1]),
    ]
    second = [
        pltpu.make_async_copy(c_hbm, c_s, load_sem.at[2]),
        pltpu.make_async_copy(gate_hbm, gate_s, load_sem.at[3]),
        pltpu.make_async_copy(gain_hbm, gain_s, load_sem.at[4]),
        pltpu.make_async_copy(skip_hbm, skip_s, skip_sem),
    ]
    for copy in first:
        copy.start()

    barrier = pltpu.get_barrier_semaphore()

    def greet(device):
        pl.semaphore_signal(barrier, inc=1, device_id=device, device_id_type=MESH)

    def report(semaphore, device):
        pl.semaphore_signal(semaphore, inc=1, device_id=device, device_id_type=MESH)

    for j in range(group):

        @pl.when((j != me_j) & (is_owner | (j % 2 == 1)))
        def _():
            greet(at_group(j))

    for y in range(rows_y):

        @pl.when(is_owner & (rank(me_y) < rank(y)))
        def _():
            greet(at_y(y))

    for z in range(nchan):

        @pl.when(me_z < z)
        def _():
            greet((me, z))

    lane = lax.broadcasted_iota(jnp.int32, (8, channels), 1)
    row8 = lax.broadcasted_iota(jnp.int32, (8, channels), 0)
    own_head = (lane // width) == row8
    half = lax.broadcasted_iota(jnp.int32, (1, LANES), 1) < width
    past = lax.broadcasted_iota(jnp.int32, (BLOCK, BLOCK), 0)
    here = lax.broadcasted_iota(jnp.int32, (BLOCK, BLOCK), 1)
    upper = jnp.where(past <= here, 1.0, 0.0).astype(BF16)
    later = jnp.where(past > here, 1.0, 0.0).astype(BF16)

    pltpu.make_async_copy(keep_step, keep_step, keep_sem).wait()
    for copy in second:
        copy.start()
    keep8[...] = jnp.zeros_like(keep8)
    step8[...] = jnp.zeros_like(step8)
    for k in range(blocks):
        keep8[8 * k : 8 * k + heads, :] = keep_step[0, :, BLOCK * k : BLOCK * (k + 1)]
        step8[8 * k : 8 * k + heads, :] = keep_step[1, :, BLOCK * k : BLOCK * (k + 1)]
    keep = keep8[...]
    k_high = keep.astype(BF16)
    k_mid, k_low = split2(keep - k_high.astype(F32))
    after = dot(k_high, later) + (dot(k_mid, later) + dot(k_low, later))
    coef8[...] = jnp.exp(after) * step8[...]

    first[2].wait()
    first[3].wait()
    cum8[...] = dot(k_high, upper) + (dot(k_mid, upper) + dot(k_low, upper))
    for k in range(blocks):
        coef = coef8[8 * k : 8 * k + 8, :]
        bt = b_s[:, BLOCK * k : BLOCK * (k + 1)].astype(F32)
        for t in range(tiles):
            lines = jnp.concatenate(
                [(bt * coef[h : h + 1, :]).astype(BF16) for h in (2 * t, 2 * t + 1)], axis=0
            )
            both = dot(lines, x_s[BLOCK * k : BLOCK * (k + 1), LANES * t : LANES * (t + 1)])
            block_state[k, :, LANES * t : LANES * (t + 1)] = jnp.where(
                half, both[:nstate], both[nstate:]
            )
    for k in range(blocks):
        last = cum8[8 * k : 8 * k + 8, BLOCK - 1 : BLOCK]
        spread = jnp.where(own_head, jnp.broadcast_to(last, (8, channels)), 0.0)
        totals[k : k + 1, :] = jnp.sum(spread, axis=0, keepdims=True)
    device_total[...] = jnp.sum(totals[...], axis=0, keepdims=True)
    running = jnp.zeros((nstate, channels), F32)
    for k in range(blocks):
        starts[k] = running
        running = jnp.exp(totals[k : k + 1, :]) * running + block_state[k]
    for q in range(group // 2):
        end_s[q] = running[piece * q : piece * (q + 1), :]

    greeted = me_z + jnp.where(is_owner, group - 1, group // 2)
    expected_y = 0
    for y in range(rows_y):
        greeted = greeted + jnp.where(is_owner & (rank(y) < rank(me_y)), 1, 0)
        expected_y = expected_y + jnp.where((y > me_y) & (rank(y) > rank(me_y)), 1, 0)
    pl.semaphore_wait(barrier, greeted)

    def copy_a(i):
        return pltpu.make_async_remote_copy(
            device_total, totals1.at[me_j], sa_send, sa_recv,
            device_id=at_group(owner((me_q + i) % (group // 2))), device_id_type=MESH,
        )

    def copy_b(i):
        q = (me_q + i) % (group // 2)
        return pltpu.make_async_remote_copy(
            end_s.at[q], gather1.at[me_j], sb_send, sb_recv,
            device_id=at_group(owner(q)), device_id_type=MESH,
        )

    others = [group // 4] + [i for i in range(group // 2) if i != group // 4]
    for i in others:

        @pl.when((i != 0) | jnp.logical_not(is_owner))
        def _():
            copy_a(i).start()
            copy_b(i).start()

    for y in range(rows_y):

        @pl.when(is_owner & (y < me_y) & (rank(y) < rank(me_y)))
        def _():
            report(y_in, at_y(y))

    for z in range(nchan):

        @pl.when(z < me_z)
        def _():
            report(z_in, (me, z))

    @pl.when(is_owner)
    def _():
        gather1[me_j] = end_s[me_q]
        totals1[me_j] = device_total[...]

    before = jnp.zeros((1, channels), F32)
    for k in range(blocks):
        prefix_s[k : k + 1, :] = before
        before = before + totals[k : k + 1, :]

    for copy in second:
        copy.wait()
    head_of = lax.broadcasted_iota(jnp.int32, (1, channels), 1) // width
    skip_row = jnp.zeros((1, channels), F32)
    for h in range(heads):
        skip_row = jnp.where(head_of == h, skip_s[0, h], skip_row)
    diagonal = (
        lax.broadcasted_iota(jnp.int32, (LANES, LANES), 0)
        >= lax.broadcasted_iota(jnp.int32, (LANES, LANES), 1)
    )

    def inside(k, carry):
        rows = pl.ds(pl.multiple_of(k * BLOCK, BLOCK), BLOCK)
        slab_at = pl.ds(pl.multiple_of(k * 8, 8), 8)
        slab = cum8[slab_at, :]
        steps = step8[slab_at, :]
        columns = jnp.transpose(slab)
        c_block = c_s[:, rows]
        c_pair = jnp.transpose(jnp.concatenate([c_block, c_block], axis=0))
        c2_s[rows, :] = c_pair
        scores = dot(c_pair[:, :nstate], b_s[:, rows])
        high, low = split2(starts[k])
        read = dot(c_pair, jnp.concatenate([high, low], axis=0))
        carried = jnp.exp(prefix_s[pl.ds(k, 1), :])
        for t in range(tiles):
            lanes = slice(LANES * t, LANES * (t + 1))
            weights, spreads = [], []
            for h in (2 * t, 2 * t + 1):
                column = jnp.broadcast_to(columns[:, h : h + 1], (BLOCK, LANES))
                spreads.append(column)

                def weight(r, s):
                    rr, ss = slice(LANES * r, LANES * (r + 1)), slice(LANES * s, LANES * (s + 1))
                    w = (
                        scores[rr, ss]
                        * jnp.exp(column[rr, :] - slab[h : h + 1, ss])
                        * steps[h : h + 1, ss]
                    )
                    return (jnp.where(diagonal, w, 0.0) if r == s else w).astype(BF16)

                top = jnp.concatenate([weight(0, 0), jnp.zeros((LANES, LANES), BF16)], axis=1)
                bottom = jnp.concatenate([weight(1, 0), weight(1, 1)], axis=1)
                weights += [top, bottom]
            x_tile = x_s[rows, lanes]
            both = dot(jnp.concatenate(weights, axis=0), x_tile)
            value = jnp.where(half, both[:BLOCK], both[BLOCK:])
            value = value + skip_row[:, lanes] * x_tile.astype(F32)
            gate = gate_s[rows, lanes].astype(F32)
            gate = gate / (1.0 + jnp.exp(-gate))
            slope = jnp.exp(jnp.where(half, spreads[0], spreads[1])) * gate
            base_s[rows, lanes] = value * gate + slope * read[:, lanes]
            slope_s[rows, lanes] = slope * carried[:, lanes]
        return carry

    third = (blocks * 3) // 8
    middle = jnp.where(me_y > 0, third + blocks // 4, third)
    lax.fori_loop(0, third, inside, 0)

    def copy_c(i):
        return pltpu.make_async_remote_copy(
            group_total, totals2.at[me_y], sc_send, sc_recv,
            device_id=at_y(me_y + i), device_id_type=MESH,
        )

    def copy_d(i):
        return pltpu.make_async_remote_copy(
            group_total_state, gather2.at[me_y], sd_send, sd_recv,
            device_id=at_y(me_y + i), device_id_type=MESH,
        )

    @pl.when(is_owner)
    def _():
        @pl.when(expected_y > 0)
        def _():
            pl.semaphore_wait(y_in, expected_y)

        arrived(totals1.at[pl.ds(0, group - 1)], sa_recv)
        total = totals1[0]
        for m in range(1, group):
            total = total + totals1[m]
        group_total[...] = total
        for i in range(1, rows_y):

            @pl.when(me_y + i < rows_y)
            def _():
                copy_c(i).start()

        arrived(gather1.at[pl.ds(0, group - 1)], sb_recv)
        state = jnp.zeros((piece, channels), F32)
        for m in range(group):
            group_prefix[m] = state
            state = jnp.exp(totals1[m]) * state + gather1[m]
        group_total_state[...] = state
        for i in sorted(range(1, rows_y), key=lambda i: -min(i, rows_y - i)):

            @pl.when(me_y + i < rows_y)
            def _():
                copy_d(i).start()


    def copy_e(i):
        p = (me_j + i) % group
        return pltpu.make_async_remote_copy(
            back_s.at[p], gather3.at[me_q], se_send, se_recv,
            device_id=at_group(p), device_id_type=MESH,
        )

    lax.fori_loop(third, middle, inside, 0)

    @pl.when(is_owner)
    def _():
        entering_s[...] = jnp.zeros_like(entering_s)
        for n in range(1, rows_y):

            @pl.when(me_y == n)
            def _():
                arrived(totals2.at[pl.ds(0, n)], sc_recv)
                arrived(gather2.at[pl.ds(0, n)], sd_recv)
                state = gather2[0]
                for y in range(1, n):
                    state = jnp.exp(totals2[y]) * state + gather2[y]
                entering_s[...] = state

        entering = entering_s[...]
        ahead = jnp.zeros((1, channels), F32)
        for m in range(group):
            back_s[m] = jnp.exp(ahead) * entering + group_prefix[m]
            ahead = ahead + totals1[m]
        for i in sorted(range(1, group), key=lambda i: i % 2 - 2 * min((i + 1) // 2, (group - i) // 2) - 3 * (i % 2)):
            copy_e(i).start()
        gather3[me_q] = back_s[me_j]

    lax.fori_loop(middle, blocks, inside, 0)

    @pl.when(is_owner)
    def _():
        arrived(gather3.at[pl.ds(0, group // 2 - 1)], se_recv)

    @pl.when(jnp.logical_not(is_owner))
    def _():
        arrived(gather3, se_recv)

    high, low = split2(jnp.concatenate([gather3[q] for q in range(group // 2)], axis=0))
    incoming = jnp.concatenate([high, low], axis=0)
    sums = jnp.zeros((BLOCK, LANES), F32)
    place = lax.broadcasted_iota(jnp.int32, (BLOCK, LANES), 1)
    for k in range(blocks):
        rows = slice(BLOCK * k, BLOCK * (k + 1))
        read = dot(c2_s[rows, :], incoming)
        gated = base_s[rows, :] + slope_s[rows, :] * read
        base_s[rows, :] = gated
        square = gated * gated
        partial = square[:, :LANES]
        for t in range(1, tiles):
            partial = partial + square[:, LANES * t : LANES * (t + 1)]
        sums = jnp.where(place == k, jnp.sum(partial, axis=1, keepdims=True), sums)
    squares_s[...] = jnp.transpose(sums)[:blocks, :]

    def copy_f(z):
        return pltpu.make_async_remote_copy(
            squares_s, gather_sq.at[me_z], sf_send, sf_recv,
            device_id=(me, z), device_id_type=MESH,
        )

    for z in range(nchan):

        @pl.when(z < me_z)
        def _():
            copy_f(z).start()

    @pl.when(me_z < nchan - 1)
    def _():
        pl.semaphore_wait(z_in, nchan - 1 - me_z)

    for z in range(nchan):

        @pl.when(z > me_z)
        def _():
            copy_f(z).start()

    gather_sq[me_z] = squares_s[...]
    for k in range(blocks):
        rows = slice(BLOCK * k, BLOCK * (k + 1))
        base_s[rows, :] = base_s[rows, :] * gain_s[...]

    arrived(gather_sq.at[pl.ds(0, nchan - 1)], sf_recv)

    total = gather_sq[0]
    for z in range(1, nchan):
        total = total + gather_sq[z]
    total_ref[...] = total

    @pl.when(is_owner)
    def _():
        sent(totals1.at[pl.ds(0, group // 2 - 1)], sa_send)
        sent(end_s.at[pl.ds(0, group // 2 - 1)], sb_send)
        sent(back_s.at[pl.ds(0, group - 1)], se_send)
        for n in range(1, rows_y):

            @pl.when(me_y == rows_y - 1 - n)
            def _():
                sent(totals2.at[pl.ds(0, n)], sc_send)
                sent(gather2.at[pl.ds(0, n)], sd_send)

    @pl.when(jnp.logical_not(is_owner))
    def _():
        sent(totals1.at[pl.ds(0, group // 2)], sa_send)
        sent(end_s, sb_send)

    sent(gather_sq.at[pl.ds(0, nchan - 1)], sf_send)


def scale_rows(width, base_ref, total_ref, out_hbm, out_s, store_sem):
    tokens, channels = base_ref.shape
    blocks = tokens // BLOCK
    factor = lax.rsqrt(total_ref[...] / width + EPSILON)
    stores = []
    for k in range(blocks):
        for r in range(BLOCK // LANES):
            rows = slice(BLOCK * k + LANES * r, BLOCK * k + LANES * (r + 1))
            line = factor[k : k + 1, LANES * r : LANES * (r + 1)]
            scale = jnp.transpose(jnp.broadcast_to(line, (LANES, LANES)))
            for t in range(channels // LANES):
                lanes = slice(LANES * t, LANES * (t + 1))
                out_s[rows, lanes] = (base_ref[rows, lanes] * scale).astype(BF16)
        rows = slice(BLOCK * k, BLOCK * (k + 1))
        store = pltpu.make_async_copy(out_s.at[rows, :], out_hbm.at[rows, :], store_sem.at[k])
        store.start()
        stores.append(store)
    for store in stores:
        store.wait()


def per_device(group, rows_y, nchan, x, gate, b, c, step, keep, skip, gain):
    tokens, channels = x.shape
    nstate = b.shape[1]
    heads = step.shape[0]
    blocks = tokens // BLOCK
    owners = group // 2
    piece = nstate // owners
    vmem = pltpu.VMEM
    dma = pltpu.SemaphoreType.DMA
    anywhere = pl.BlockSpec(memory_space=pl.ANY)
    operands = (x, gate, b.T, c.T, step, keep, skip.reshape(1, heads), gain.reshape(1, channels))
    scratch = [
        vmem((tokens, channels), BF16), vmem((tokens, channels), BF16),
        vmem((nstate, tokens), BF16), vmem((nstate, tokens), BF16),
        vmem((2, heads, tokens), F32),
        pltpu.SMEM((1, heads), F32), vmem((1, channels), F32),
        vmem((8 * blocks, BLOCK), F32), vmem((8 * blocks, BLOCK), F32),
        vmem((8 * blocks, BLOCK), F32), vmem((8 * blocks, BLOCK), F32),
        vmem((tokens, 2 * nstate), BF16),
        vmem((blocks, channels), F32), vmem((1, channels), F32),
        vmem((blocks, nstate, channels), F32), vmem((blocks, nstate, channels), F32),
        vmem((blocks, channels), F32),
        vmem((owners, piece, channels), F32), vmem((group, piece, channels), F32),
        vmem((group, 1, channels), F32), vmem((group, piece, channels), F32),
        vmem((piece, channels), F32), vmem((1, channels), F32),
        vmem((rows_y, piece, channels), F32), vmem((rows_y, 1, channels), F32),
        vmem((piece, channels), F32),
        vmem((group, piece, channels), F32), vmem((owners, piece, channels), F32),
        vmem((tokens, channels), F32),
        vmem((blocks, BLOCK), F32), vmem((nchan, blocks, BLOCK), F32),
        dma((5,)), dma, dma, pltpu.SemaphoreType.REGULAR, pltpu.SemaphoreType.REGULAR,
    ] + [dma] * 12
    base, total = pl.pallas_call(
        functools.partial(layer, group, rows_y, nchan),
        out_shape=(
            jax.ShapeDtypeStruct((tokens, channels), F32),
            jax.ShapeDtypeStruct((blocks, BLOCK), F32),
        ),
        in_specs=[anywhere] * 8,
        out_specs=(pl.BlockSpec(memory_space=pltpu.VMEM),) * 2,
        scratch_shapes=scratch,
        compiler_params=pltpu.CompilerParams(
            collective_id=0, has_side_effects=True, vmem_limit_bytes=24 * 1024 * 1024
        ),
    )(*[pltpu.with_memory_space_constraint(v, pltpu.HBM) for v in operands])
    return pl.pallas_call(
        functools.partial(scale_rows, channels * nchan),
        out_shape=jax.ShapeDtypeStruct((tokens, channels), BF16),
        in_specs=[pl.BlockSpec(memory_space=pltpu.VMEM)] * 2,
        out_specs=anywhere,
        scratch_shapes=[vmem((tokens, channels), BF16), dma((blocks,))],
        compiler_params=pltpu.CompilerParams(vmem_limit_bytes=8 * 1024 * 1024),
    )(base, total)


def build(mesh, group):
    rows_y = mesh.shape["seq"] // group
    placed = (
        P("seq", "chan"), P("seq", "chan"), P("seq", None), P("seq", None),
        P("chan", "seq"), P("chan", "seq"), P("chan"), P("chan"),
    )
    return jax.shard_map(
        functools.partial(per_device, group, rows_y, mesh.shape["chan"]),
        mesh=mesh, in_specs=placed, out_specs=P("seq", "chan"), check_vma=False,
    )


def solution(mesh):
    return build(mesh, GROUP)
```

```python
import functools

import jax
import jax.numpy as jnp
from jax import lax
from jax.experimental import pallas as pl
from jax.experimental.pallas import tpu as pltpu
from jax.sharding import PartitionSpec as P

BLOCK = 256
LANES = 128
EPSILON = 1e-05
GROUP = 8
MESH = pl.DeviceIdType.MESH
F32 = jnp.float32
BF16 = jnp.bfloat16


def split2(v):
    high = v.astype(BF16)
    return high, (v - high.astype(F32)).astype(BF16)


def dot(a, b, contract=((1,), (0,))):
    return lax.dot_general(a, b, (contract, ((), ())), preferred_element_type=F32)


def layer(
    group, rows_y, nchan,
    x_hbm, gate_hbm, b_hbm, c_hbm, step_hbm, keep_hbm, skip_hbm, gain_hbm,
    base_s, total_ref,
    x_s, gate_s, b_s, c_s, keep_step, skip_s, gain_s,
    keep8, step8, coef8, cum8, c2_s,
    totals, device_total, block_state, starts, prefix_s,
    end_s, gather1, totals1, group_prefix, group_total_state, group_total,
    gather2, totals2, entering_s, back_s, gather3,
    slope_s, squares_s, gather_sq, lines_s,
    load_sem, keep_sem, skip_sem, y_in, z_in,
    send_sem, b_recv, d_recv, e_recv, f_recv,
):
    tokens, channels = x_s.shape
    nstate = b_s.shape[0]
    heads = keep_step.shape[1]
    width = channels // heads
    blocks = tokens // BLOCK
    tiles = channels // LANES
    per_tile = heads // tiles
    piece = 2 * nstate // group

    me = lax.axis_index("seq")
    me_z = lax.axis_index("chan")
    me_y = me // group
    me_j = me % group
    is_owner = me_j % 2 == 1
    me_q = me_j // 2

    def owner(q):
        return 2 * q + 1

    def at_group(j):
        return (me_y * group + j, me_z)

    def at_y(y):
        return (y * group + me_j, me_z)

    def lines_of(count, semaphore):
        ref = lines_s.at[pl.ds(0, count)]
        return pltpu.make_async_remote_copy(
            ref, ref, semaphore, semaphore,
            device_id=(me, (me_z + 1) % nchan), device_id_type=MESH,
        )

    def arrived(count, semaphore):
        lines_of(count, semaphore).wait_recv()

    def sent(count):
        lines_of(count, send_sem).wait_send()

    owners = group // 2

    def rank(y):
        return jnp.minimum(y, rows_y - y) * rows_y + y

    first = [
        pltpu.make_async_copy(keep_hbm, keep_step.at[0], keep_sem),
        pltpu.make_async_copy(step_hbm, keep_step.at[1], keep_sem),
        pltpu.make_async_copy(b_hbm, b_s, load_sem.at[0]),
        pltpu.make_async_copy(x_hbm, x_s, load_sem.at[1]),
    ]
    second = [
        pltpu.make_async_copy(c_hbm, c_s, load_sem.at[2]),
        pltpu.make_async_copy(gate_hbm, gate_s, load_sem.at[3]),
        pltpu.make_async_copy(gain_hbm, gain_s, load_sem.at[4]),
        pltpu.make_async_copy(skip_hbm, skip_s, skip_sem),
    ]
    for copy in first:
        copy.start()

    barrier = pltpu.get_barrier_semaphore()

    def greet(device):
        pl.semaphore_signal(barrier, inc=1, device_id=device, device_id_type=MESH)

    def report(semaphore, device):
        pl.semaphore_signal(semaphore, inc=1, device_id=device, device_id_type=MESH)

    for j in range(group):

        @pl.when((j != me_j) & (is_owner | (j % 2 == 1)))
        def _():
            greet(at_group(j))

    for y in range(rows_y):

        @pl.when(is_owner & (rank(me_y) < rank(y)))
        def _():
            greet(at_y(y))

    for z in range(nchan):

        @pl.when(me_z < z)
        def _():
            greet((me, z))

    lane = lax.broadcasted_iota(jnp.int32, (8, channels), 1)
    row8 = lax.broadcasted_iota(jnp.int32, (8, channels), 0)
    own_head = (lane // width) == row8
    half = lax.broadcasted_iota(jnp.int32, (1, LANES), 1) < width
    past = lax.broadcasted_iota(jnp.int32, (BLOCK, BLOCK), 0)
    here = lax.broadcasted_iota(jnp.int32, (BLOCK, BLOCK), 1)
    upper = jnp.where(past <= here, 1.0, 0.0).astype(BF16)
    later = jnp.where(past > here, 1.0, 0.0).astype(BF16)

    pltpu.make_async_copy(keep_step, keep_step, keep_sem).wait()
    for copy in second:
        copy.start()
    keep8[...] = jnp.zeros_like(keep8)
    step8[...] = jnp.zeros_like(step8)
    for k in range(blocks):
        keep8[8 * k : 8 * k + heads, :] = keep_step[0, :, BLOCK * k : BLOCK * (k + 1)]
        step8[8 * k : 8 * k + heads, :] = keep_step[1, :, BLOCK * k : BLOCK * (k + 1)]
    keep = keep8[...]
    k_high = keep.astype(BF16)
    k_mid, k_low = split2(keep - k_high.astype(F32))
    after = dot(k_high, later) + (dot(k_mid, later) + dot(k_low, later))
    coef8[...] = jnp.exp(after) * step8[...]

    first[2].wait()
    first[3].wait()
    cum8[...] = dot(k_high, upper) + (dot(k_mid, upper) + dot(k_low, upper))
    for k in range(blocks):
        coef = coef8[8 * k : 8 * k + 8, :]
        bt = b_s[:, BLOCK * k : BLOCK * (k + 1)].astype(F32)
        for t in range(tiles):
            lines = jnp.concatenate(
                [(bt * coef[h : h + 1, :]).astype(BF16) for h in (2 * t, 2 * t + 1)], axis=0
            )
            both = dot(lines, x_s[BLOCK * k : BLOCK * (k + 1), LANES * t : LANES * (t + 1)])
            block_state[k, :, LANES * t : LANES * (t + 1)] = jnp.where(
                half, both[:nstate], both[nstate:]
            )
    for k in range(blocks):
        last = cum8[8 * k : 8 * k + 8, BLOCK - 1 : BLOCK]
        spread = jnp.where(own_head, jnp.broadcast_to(last, (8, channels)), 0.0)
        totals[k : k + 1, :] = jnp.sum(spread, axis=0, keepdims=True)
    device_total[...] = jnp.sum(totals[...], axis=0, keepdims=True)
    running = jnp.zeros((nstate, channels), F32)
    for k in range(blocks):
        starts[k] = running
        running = jnp.exp(totals[k : k + 1, :]) * running + block_state[k]
    for q in range(group // 2):
        end_s[q] = running[piece * q : piece * (q + 1), :]

    greeted = me_z + jnp.where(is_owner, group - 1, group // 2)
    expected_y = 0
    for y in range(rows_y):
        greeted = greeted + jnp.where(is_owner & (rank(y) < rank(me_y)), 1, 0)
        expected_y = expected_y + jnp.where((y > me_y) & (rank(y) > rank(me_y)), 1, 0)
    pl.semaphore_wait(barrier, greeted)

    def copy_a(i):
        return pltpu.make_async_remote_copy(
            device_total, totals1.at[me_j], send_sem, b_recv,
            device_id=at_group(owner((me_q + i) % (group // 2))), device_id_type=MESH,
        )

    def copy_b(i):
        q = (me_q + i) % (group // 2)
        return pltpu.make_async_remote_copy(
            end_s.at[q], gather1.at[me_j], send_sem, b_recv,
            device_id=at_group(owner(q)), device_id_type=MESH,
        )

    others = [group // 4] + [i for i in range(group // 2) if i != group // 4]
    for i in others:

        @pl.when((i != 0) | jnp.logical_not(is_owner))
        def _():
            copy_a(i).start()
            copy_b(i).start()

    for y in range(rows_y):

        @pl.when(is_owner & (y < me_y) & (rank(y) < rank(me_y)))
        def _():
            report(y_in, at_y(y))

    for z in range(nchan):

        @pl.when(z < me_z)
        def _():
            report(z_in, (me, z))

    @pl.when(is_owner)
    def _():
        gather1[me_j] = end_s[me_q]
        totals1[me_j] = device_total[...]

    before = jnp.zeros((1, channels), F32)
    for k in range(blocks):
        prefix_s[k : k + 1, :] = before
        before = before + totals[k : k + 1, :]

    for copy in second:
        copy.wait()
    head_of = lax.broadcasted_iota(jnp.int32, (1, channels), 1) // width
    skip_row = jnp.zeros((1, channels), F32)
    for h in range(heads):
        skip_row = jnp.where(head_of == h, skip_s[0, h], skip_row)
    diagonal = (
        lax.broadcasted_iota(jnp.int32, (LANES, LANES), 0)
        >= lax.broadcasted_iota(jnp.int32, (LANES, LANES), 1)
    )

    def inside(k, carry):
        rows = pl.ds(pl.multiple_of(k * BLOCK, BLOCK), BLOCK)
        slab_at = pl.ds(pl.multiple_of(k * 8, 8), 8)
        slab = cum8[slab_at, :]
        steps = step8[slab_at, :]
        columns = jnp.transpose(slab)
        c_block = c_s[:, rows]
        c_pair = jnp.transpose(jnp.concatenate([c_block, c_block], axis=0))
        c2_s[rows, :] = c_pair
        scores = dot(c_pair[:, :nstate], b_s[:, rows])
        high, low = split2(starts[k])
        read = dot(c_pair, jnp.concatenate([high, low], axis=0))
        carried = jnp.exp(prefix_s[pl.ds(k, 1), :])
        for t in range(tiles):
            lanes = slice(LANES * t, LANES * (t + 1))
            weights, spreads = [], []
            for h in (2 * t, 2 * t + 1):
                column = jnp.broadcast_to(columns[:, h : h + 1], (BLOCK, LANES))
                spreads.append(column)

                def weight(r, s):
                    rr, ss = slice(LANES * r, LANES * (r + 1)), slice(LANES * s, LANES * (s + 1))
                    w = (
                        scores[rr, ss]
                        * jnp.exp(column[rr, :] - slab[h : h + 1, ss])
                        * steps[h : h + 1, ss]
                    )
                    return (jnp.where(diagonal, w, 0.0) if r == s else w).astype(BF16)

                top = jnp.concatenate([weight(0, 0), jnp.zeros((LANES, LANES), BF16)], axis=1)
                bottom = jnp.concatenate([weight(1, 0), weight(1, 1)], axis=1)
                weights += [top, bottom]
            x_tile = x_s[rows, lanes]
            both = dot(jnp.concatenate(weights, axis=0), x_tile)
            value = jnp.where(half, both[:BLOCK], both[BLOCK:])
            value = value + skip_row[:, lanes] * x_tile.astype(F32)
            gate = gate_s[rows, lanes].astype(F32)
            gate = gate / (1.0 + jnp.exp(-gate))
            slope = jnp.exp(jnp.where(half, spreads[0], spreads[1])) * gate
            base_s[rows, lanes] = value * gate + slope * read[:, lanes]
            slope_s[rows, lanes] = slope * carried[:, lanes]
        return carry

    third = (blocks * 3) // 8
    middle = jnp.where(me_y > 0, third + blocks // 4, third)
    lax.fori_loop(0, third, inside, 0)

    def copy_c(i):
        return pltpu.make_async_remote_copy(
            group_total, totals2.at[me_y], send_sem, d_recv,
            device_id=at_y(me_y + i), device_id_type=MESH,
        )

    def copy_d(i):
        return pltpu.make_async_remote_copy(
            group_total_state, gather2.at[me_y], send_sem, d_recv,
            device_id=at_y(me_y + i), device_id_type=MESH,
        )

    @pl.when(is_owner)
    def _():
        @pl.when(expected_y > 0)
        def _():
            pl.semaphore_wait(y_in, expected_y)

        arrived((group - 1) * (piece + 1), b_recv)
        total = totals1[0]
        for m in range(1, group):
            total = total + totals1[m]
        group_total[...] = total
        for i in range(1, rows_y):

            @pl.when(me_y + i < rows_y)
            def _():
                copy_c(i).start()

        state = jnp.zeros((piece, channels), F32)
        for m in range(group):
            group_prefix[m] = state
            state = jnp.exp(totals1[m]) * state + gather1[m]
        group_total_state[...] = state
        for i in sorted(range(1, rows_y), key=lambda i: -min(i, rows_y - i)):

            @pl.when(me_y + i < rows_y)
            def _():
                copy_d(i).start()


    def copy_e(i):
        p = (me_j + i) % group
        return pltpu.make_async_remote_copy(
            back_s.at[p], gather3.at[me_q], send_sem, e_recv,
            device_id=at_group(p), device_id_type=MESH,
        )

    lax.fori_loop(third, middle, inside, 0)

    @pl.when(is_owner)
    def _():
        entering_s[...] = jnp.zeros_like(entering_s)
        for n in range(1, rows_y):

            @pl.when(me_y == n)
            def _():
                arrived(n * (piece + 1), d_recv)
                state = gather2[0]
                for y in range(1, n):
                    state = jnp.exp(totals2[y]) * state + gather2[y]
                entering_s[...] = state

        entering = entering_s[...]
        ahead = jnp.zeros((1, channels), F32)
        for m in range(group):
            back_s[m] = jnp.exp(ahead) * entering + group_prefix[m]
            ahead = ahead + totals1[m]
        for i in sorted(range(1, group), key=lambda i: i % 2 - 2 * min((i + 1) // 2, (group - i) // 2) - 3 * (i % 2)):
            copy_e(i).start()
        gather3[me_q] = back_s[me_j]

    lax.fori_loop(middle, blocks, inside, 0)

    @pl.when(is_owner)
    def _():
        arrived((owners - 1) * piece, e_recv)

    @pl.when(jnp.logical_not(is_owner))
    def _():
        arrived(owners * piece, e_recv)

    high, low = split2(jnp.concatenate([gather3[q] for q in range(group // 2)], axis=0))
    incoming = jnp.concatenate([high, low], axis=0)
    sums = jnp.zeros((BLOCK, LANES), F32)
    place = lax.broadcasted_iota(jnp.int32, (BLOCK, LANES), 1)
    for k in range(blocks):
        rows = slice(BLOCK * k, BLOCK * (k + 1))
        read = dot(c2_s[rows, :], incoming)
        gated = base_s[rows, :] + slope_s[rows, :] * read
        base_s[rows, :] = gated
        square = gated * gated
        partial = square[:, :LANES]
        for t in range(1, tiles):
            partial = partial + square[:, LANES * t : LANES * (t + 1)]
        sums = jnp.where(place == k, jnp.sum(partial, axis=1, keepdims=True), sums)
    squares_s[...] = jnp.transpose(sums)[:blocks, :]

    def copy_f(z):
        return pltpu.make_async_remote_copy(
            squares_s, gather_sq.at[me_z], send_sem, f_recv,
            device_id=(me, z), device_id_type=MESH,
        )

    for z in range(nchan):

        @pl.when(z < me_z)
        def _():
            copy_f(z).start()

    @pl.when(me_z < nchan - 1)
    def _():
        pl.semaphore_wait(z_in, nchan - 1 - me_z)

    for z in range(nchan):

        @pl.when(z > me_z)
        def _():
            copy_f(z).start()

    gather_sq[me_z] = squares_s[...]
    for k in range(blocks):
        rows = slice(BLOCK * k, BLOCK * (k + 1))
        base_s[rows, :] = base_s[rows, :] * gain_s[...]

    arrived((nchan - 1) * blocks, f_recv)

    total = gather_sq[0]
    for z in range(1, nchan):
        total = total + gather_sq[z]
    total_ref[...] = total

    for n in range(rows_y):

        @pl.when(is_owner & (me_y == rows_y - 1 - n))
        def _():
            sent((owners - 1 + n) * (piece + 1) + (group - 1) * piece + (nchan - 1) * blocks)

    @pl.when(jnp.logical_not(is_owner))
    def _():
        sent(owners * (piece + 1) + (nchan - 1) * blocks)


def scale_rows(width, base_ref, total_ref, out_hbm, out_s, store_sem):
    tokens, channels = base_ref.shape
    blocks = tokens // BLOCK
    factor = lax.rsqrt(total_ref[...] / width + EPSILON)
    for k in range(blocks):
        for r in range(BLOCK // LANES):
            part = slice(LANES * r, LANES * (r + 1))
            rows = slice(BLOCK * k + LANES * r, BLOCK * k + LANES * (r + 1))
            scale = jnp.transpose(jnp.broadcast_to(factor[k : k + 1, part], (LANES, LANES)))
            for t in range(channels // LANES):
                lanes = slice(LANES * t, LANES * (t + 1))
                out_s[rows, lanes] = (base_ref[rows, lanes] * scale).astype(BF16)
        rows = slice(BLOCK * k, BLOCK * (k + 1))
        pltpu.make_async_copy(out_s.at[rows, :], out_hbm.at[rows, :], store_sem).start()
    pltpu.make_async_copy(out_s, out_hbm, store_sem).wait()


def per_device(group, rows_y, nchan, x, gate, b, c, step, keep, skip, gain):
    tokens, channels = x.shape
    nstate = b.shape[1]
    heads = step.shape[0]
    blocks = tokens // BLOCK
    owners = group // 2
    piece = nstate // owners
    vmem = pltpu.VMEM
    dma = pltpu.SemaphoreType.DMA
    anywhere = pl.BlockSpec(memory_space=pl.ANY)
    operands = (x, gate, b.T, c.T, step, keep, skip.reshape(1, heads), gain.reshape(1, channels))
    scratch = [
        vmem((tokens, channels), BF16), vmem((tokens, channels), BF16),
        vmem((nstate, tokens), BF16), vmem((nstate, tokens), BF16),
        vmem((2, heads, tokens), F32),
        pltpu.SMEM((1, heads), F32), vmem((1, channels), F32),
        vmem((8 * blocks, BLOCK), F32), vmem((8 * blocks, BLOCK), F32),
        vmem((8 * blocks, BLOCK), F32), vmem((8 * blocks, BLOCK), F32),
        vmem((tokens, 2 * nstate), BF16),
        vmem((blocks, channels), F32), vmem((1, channels), F32),
        vmem((blocks, nstate, channels), F32), vmem((blocks, nstate, channels), F32),
        vmem((blocks, channels), F32),
        vmem((owners, piece, channels), F32), vmem((group, piece, channels), F32),
        vmem((group, 1, channels), F32), vmem((group, piece, channels), F32),
        vmem((piece, channels), F32), vmem((1, channels), F32),
        vmem((rows_y, piece, channels), F32), vmem((rows_y, 1, channels), F32),
        vmem((piece, channels), F32),
        vmem((group, piece, channels), F32), vmem((owners, piece, channels), F32),
        vmem((tokens, channels), F32),
        vmem((blocks, BLOCK), F32), vmem((nchan, blocks, BLOCK), F32),
        vmem(((owners + rows_y) * (piece + 1) + group * piece + nchan * blocks, 1, channels), F32),
        dma((5,)), dma, dma, pltpu.SemaphoreType.REGULAR, pltpu.SemaphoreType.REGULAR,
    ] + [dma] * 5
    base, total = pl.pallas_call(
        functools.partial(layer, group, rows_y, nchan),
        out_shape=(
            jax.ShapeDtypeStruct((tokens, channels), F32),
            jax.ShapeDtypeStruct((blocks, BLOCK), F32),
        ),
        in_specs=[anywhere] * 8,
        out_specs=(pl.BlockSpec(memory_space=pltpu.VMEM),) * 2,
        scratch_shapes=scratch,
        compiler_params=pltpu.CompilerParams(
            collective_id=0, has_side_effects=True, vmem_limit_bytes=24 * 1024 * 1024
        ),
    )(*[pltpu.with_memory_space_constraint(v, pltpu.HBM) for v in operands])
    return pl.pallas_call(
        functools.partial(scale_rows, channels * nchan),
        out_shape=jax.ShapeDtypeStruct((tokens, channels), BF16),
        in_specs=[pl.BlockSpec(memory_space=pltpu.VMEM)] * 2,
        out_specs=anywhere,
        scratch_shapes=[vmem((tokens, channels), BF16), dma],
        compiler_params=pltpu.CompilerParams(vmem_limit_bytes=8 * 1024 * 1024),
    )(base, total)


def build(mesh, group):
    rows_y = mesh.shape["seq"] // group
    placed = (
        P("seq", "chan"), P("seq", "chan"), P("seq", None), P("seq", None),
        P("chan", "seq"), P("chan", "seq"), P("chan"), P("chan"),
    )
    return jax.shard_map(
        functools.partial(per_device, group, rows_y, mesh.shape["chan"]),
        mesh=mesh, in_specs=placed, out_specs=P("seq", "chan"), check_vma=False,
    )


def solution(mesh):
    return build(mesh, GROUP)
```

```python
import functools

import jax
import jax.numpy as jnp
from jax import lax
from jax.experimental import pallas as pl
from jax.experimental.pallas import tpu as pltpu
from jax.sharding import PartitionSpec as P

BLOCK = 256
LANES = 128
EPSILON = 1e-05
GROUP = 8
MESH = pl.DeviceIdType.MESH
F32 = jnp.float32
BF16 = jnp.bfloat16


def split2(v):
    high = v.astype(BF16)
    return high, (v - high.astype(F32)).astype(BF16)


def dot(a, b, contract=((1,), (0,))):
    return lax.dot_general(a, b, (contract, ((), ())), preferred_element_type=F32)


def layer(
    group, rows_y, nchan,
    x_hbm, gate_hbm, b_hbm, c_hbm, step_hbm, keep_hbm, skip_hbm, gain_hbm,
    base_s, total_ref,
    x_s, gate_s, b_s, c_s, keep_step, skip_s, gain_s,
    keep8, step8, coef8, cum8, c2_s,
    totals, device_total, block_state, starts, prefix_s,
    end_s, gather1, totals1, group_prefix, group_total_state, group_total,
    gather2, totals2, entering_s, back_s, gather3,
    slope_s, squares_s, gather_sq, lines_s,
    load_sem, keep_sem, skip_sem, y_in, z_in,
    send_sem, b_recv, d_recv, e_recv, f_recv,
):
    tokens, channels = x_s.shape
    nstate = b_s.shape[0]
    heads = keep_step.shape[1]
    width = channels // heads
    blocks = tokens // BLOCK
    tiles = channels // LANES
    per_tile = heads // tiles
    piece = 2 * nstate // group

    me = lax.axis_index("seq")
    me_z = lax.axis_index("chan")
    me_y = me // group
    me_j = me % group
    is_owner = me_j % 2 == 1
    me_q = me_j // 2

    def owner(q):
        return 2 * q + 1

    def at_group(j):
        return (me_y * group + j, me_z)

    def at_y(y):
        return (y * group + me_j, me_z)

    def lines_of(count, semaphore):
        ref = lines_s.at[pl.ds(0, count)]
        return pltpu.make_async_remote_copy(
            ref, ref, semaphore, semaphore,
            device_id=(me, (me_z + 1) % nchan), device_id_type=MESH,
        )

    def arrived(count, semaphore):
        lines_of(count, semaphore).wait_recv()

    def sent(count):
        lines_of(count, send_sem).wait_send()

    owners = group // 2

    def rank(y):
        return jnp.minimum(y, rows_y - y) * rows_y + y

    by_rank = sorted(range(rows_y), key=lambda y: min(y, rows_y - y) * rows_y + y)

    first = [
        pltpu.make_async_copy(keep_hbm, keep_step.at[0], keep_sem),
        pltpu.make_async_copy(step_hbm, keep_step.at[1], keep_sem),
        pltpu.make_async_copy(b_hbm, b_s, load_sem.at[0]),
        pltpu.make_async_copy(x_hbm, x_s, load_sem.at[1]),
    ]
    second = [
        pltpu.make_async_copy(c_hbm, c_s, load_sem.at[2]),
        pltpu.make_async_copy(gate_hbm, gate_s, load_sem.at[3]),
        pltpu.make_async_copy(gain_hbm, gain_s, load_sem.at[4]),
        pltpu.make_async_copy(skip_hbm, skip_s, skip_sem),
    ]
    for copy in first:
        copy.start()

    barrier = pltpu.get_barrier_semaphore()

    def greet(device):
        pl.semaphore_signal(barrier, inc=1, device_id=device, device_id_type=MESH)

    def report(semaphore, device):
        pl.semaphore_signal(semaphore, inc=1, device_id=device, device_id_type=MESH)

    for j in range(group):

        @pl.when((j != me_j) & (is_owner | (j % 2 == 1)))
        def _():
            greet(at_group(j))

    for y in range(rows_y):

        @pl.when(is_owner & (rank(me_y) < rank(y)))
        def _():
            greet(at_y(y))

    for z in range(nchan):

        @pl.when(me_z < z)
        def _():
            greet((me, z))

    lane = lax.broadcasted_iota(jnp.int32, (8, channels), 1)
    row8 = lax.broadcasted_iota(jnp.int32, (8, channels), 0)
    own_head = (lane // width) == row8
    half = lax.broadcasted_iota(jnp.int32, (1, LANES), 1) < width
    past = lax.broadcasted_iota(jnp.int32, (BLOCK, BLOCK), 0)
    here = lax.broadcasted_iota(jnp.int32, (BLOCK, BLOCK), 1)
    upper = jnp.where(past <= here, 1.0, 0.0).astype(BF16)
    later = jnp.where(past > here, 1.0, 0.0).astype(BF16)

    pltpu.make_async_copy(keep_step, keep_step, keep_sem).wait()
    for copy in second:
        copy.start()
    keep8[...] = jnp.zeros_like(keep8)
    step8[...] = jnp.zeros_like(step8)
    for k in range(blocks):
        keep8[8 * k : 8 * k + heads, :] = keep_step[0, :, BLOCK * k : BLOCK * (k + 1)]
        step8[8 * k : 8 * k + heads, :] = keep_step[1, :, BLOCK * k : BLOCK * (k + 1)]
    keep = keep8[...]
    k_high = keep.astype(BF16)
    k_mid, k_low = split2(keep - k_high.astype(F32))
    after = dot(k_high, later) + (dot(k_mid, later) + dot(k_low, later))
    coef8[...] = jnp.exp(after) * step8[...]

    first[2].wait()
    first[3].wait()
    cum8[...] = dot(k_high, upper) + (dot(k_mid, upper) + dot(k_low, upper))
    for k in range(blocks):
        coef = coef8[8 * k : 8 * k + 8, :]
        bt = b_s[:, BLOCK * k : BLOCK * (k + 1)].astype(F32)
        for t in range(tiles):
            lines = jnp.concatenate(
                [(bt * coef[h : h + 1, :]).astype(BF16) for h in (2 * t, 2 * t + 1)], axis=0
            )
            both = dot(lines, x_s[BLOCK * k : BLOCK * (k + 1), LANES * t : LANES * (t + 1)])
            block_state[k, :, LANES * t : LANES * (t + 1)] = jnp.where(
                half, both[:nstate], both[nstate:]
            )
    for k in range(blocks):
        last = cum8[8 * k : 8 * k + 8, BLOCK - 1 : BLOCK]
        spread = jnp.where(own_head, jnp.broadcast_to(last, (8, channels)), 0.0)
        totals[k : k + 1, :] = jnp.sum(spread, axis=0, keepdims=True)
    device_total[...] = jnp.sum(totals[...], axis=0, keepdims=True)
    running = jnp.zeros((nstate, channels), F32)
    for k in range(blocks):
        starts[k] = running
        running = jnp.exp(totals[k : k + 1, :]) * running + block_state[k]
    for q in range(group // 2):
        end_s[q] = running[piece * q : piece * (q + 1), :]

    greeted = me_z + jnp.where(is_owner, group - 1, group // 2)
    for y in range(rows_y):
        greeted = greeted + jnp.where(is_owner & (rank(y) < rank(me_y)), 1, 0)
    pl.semaphore_wait(barrier, greeted)

    def copy_a(i):
        return pltpu.make_async_remote_copy(
            device_total, totals1.at[me_j], send_sem, b_recv,
            device_id=at_group(owner((me_q + i) % (group // 2))), device_id_type=MESH,
        )

    def copy_b(i):
        q = (me_q + i) % (group // 2)
        return pltpu.make_async_remote_copy(
            end_s.at[q], gather1.at[me_j], send_sem, b_recv,
            device_id=at_group(owner(q)), device_id_type=MESH,
        )

    others = [group // 4] + [i for i in range(group // 2) if i != group // 4]
    for i in others:

        @pl.when((i != 0) | jnp.logical_not(is_owner))
        def _():
            copy_a(i).start()
            copy_b(i).start()

    for y in range(rows_y):

        @pl.when(is_owner & (y < me_y) & (rank(y) < rank(me_y)))
        def _():
            report(y_in.at[me_y], at_y(y))

    for z in range(nchan):

        @pl.when(z < me_z)
        def _():
            report(z_in, (me, z))

    @pl.when(is_owner)
    def _():
        gather1[me_j] = end_s[me_q]
        totals1[me_j] = device_total[...]

    before = jnp.zeros((1, channels), F32)
    for k in range(blocks):
        prefix_s[k : k + 1, :] = before
        before = before + totals[k : k + 1, :]

    for copy in second:
        copy.wait()
    head_of = lax.broadcasted_iota(jnp.int32, (1, channels), 1) // width
    skip_row = jnp.zeros((1, channels), F32)
    for h in range(heads):
        skip_row = jnp.where(head_of == h, skip_s[0, h], skip_row)
    diagonal = (
        lax.broadcasted_iota(jnp.int32, (LANES, LANES), 0)
        >= lax.broadcasted_iota(jnp.int32, (LANES, LANES), 1)
    )

    def inside(k, carry):
        rows = pl.ds(pl.multiple_of(k * BLOCK, BLOCK), BLOCK)
        slab_at = pl.ds(pl.multiple_of(k * 8, 8), 8)
        slab = cum8[slab_at, :]
        steps = step8[slab_at, :]
        columns = jnp.transpose(slab)
        c_block = c_s[:, rows]
        c_pair = jnp.transpose(jnp.concatenate([c_block, c_block], axis=0))
        c2_s[rows, :] = c_pair
        scores = dot(c_pair[:, :nstate], b_s[:, rows])
        high, low = split2(starts[k])
        read = dot(c_pair, jnp.concatenate([high, low], axis=0))
        carried = jnp.exp(prefix_s[pl.ds(k, 1), :])
        for t in range(tiles):
            lanes = slice(LANES * t, LANES * (t + 1))
            weights, spreads = [], []
            for h in (2 * t, 2 * t + 1):
                column = jnp.broadcast_to(columns[:, h : h + 1], (BLOCK, LANES))
                spreads.append(column)

                def weight(r, s):
                    rr, ss = slice(LANES * r, LANES * (r + 1)), slice(LANES * s, LANES * (s + 1))
                    w = (
                        scores[rr, ss]
                        * jnp.exp(column[rr, :] - slab[h : h + 1, ss])
                        * steps[h : h + 1, ss]
                    )
                    return (jnp.where(diagonal, w, 0.0) if r == s else w).astype(BF16)

                top = jnp.concatenate([weight(0, 0), jnp.zeros((LANES, LANES), BF16)], axis=1)
                bottom = jnp.concatenate([weight(1, 0), weight(1, 1)], axis=1)
                weights += [top, bottom]
            x_tile = x_s[rows, lanes]
            both = dot(jnp.concatenate(weights, axis=0), x_tile)
            value = jnp.where(half, both[:BLOCK], both[BLOCK:])
            value = value + skip_row[:, lanes] * x_tile.astype(F32)
            gate = gate_s[rows, lanes].astype(F32)
            gate = gate / (1.0 + jnp.exp(-gate))
            slope = jnp.exp(jnp.where(half, spreads[0], spreads[1])) * gate
            base_s[rows, lanes] = value * gate + slope * read[:, lanes]
            slope_s[rows, lanes] = slope * carried[:, lanes]
        return carry

    third = (blocks * 3) // 8
    middle = jnp.where(me_y > 0, third + blocks // 4, third)
    lax.fori_loop(0, third, inside, 0)

    def copy_c(y):
        return pltpu.make_async_remote_copy(
            group_total, totals2.at[me_y], send_sem, d_recv,
            device_id=at_y(y), device_id_type=MESH,
        )

    def copy_d(y):
        return pltpu.make_async_remote_copy(
            group_total_state, gather2.at[me_y], send_sem, d_recv,
            device_id=at_y(y), device_id_type=MESH,
        )

    @pl.when(is_owner)
    def _():
        arrived((group - 1) * (piece + 1), b_recv)
        total = totals1[0]
        for m in range(1, group):
            total = total + totals1[m]
        group_total[...] = total
        state = jnp.zeros((piece, channels), F32)
        for m in range(group):
            group_prefix[m] = state
            state = jnp.exp(totals1[m]) * state + gather1[m]
        group_total_state[...] = state
        for y in by_rank:

            @pl.when((y > me_y) & (rank(me_y) < rank(y)))
            def _():
                pl.semaphore_wait(y_in.at[y], 1)

            @pl.when(y > me_y)
            def _():
                copy_c(y).start()
                copy_d(y).start()

    def copy_e(i):
        p = (me_j + i) % group
        return pltpu.make_async_remote_copy(
            back_s.at[p], gather3.at[me_q], send_sem, e_recv,
            device_id=at_group(p), device_id_type=MESH,
        )

    lax.fori_loop(third, middle, inside, 0)

    @pl.when(is_owner)
    def _():
        entering_s[...] = jnp.zeros_like(entering_s)
        for n in range(1, rows_y):

            @pl.when(me_y == n)
            def _():
                arrived(n * (piece + 1), d_recv)
                state = gather2[0]
                for y in range(1, n):
                    state = jnp.exp(totals2[y]) * state + gather2[y]
                entering_s[...] = state

        entering = entering_s[...]
        ahead = jnp.zeros((1, channels), F32)
        for m in range(group):
            back_s[m] = jnp.exp(ahead) * entering + group_prefix[m]
            ahead = ahead + totals1[m]
        for i in sorted(range(1, group), key=lambda i: i % 2 - 2 * min((i + 1) // 2, (group - i) // 2) - 3 * (i % 2)):
            copy_e(i).start()
        gather3[me_q] = back_s[me_j]

    lax.fori_loop(middle, blocks, inside, 0)

    @pl.when(is_owner)
    def _():
        arrived((owners - 1) * piece, e_recv)

    @pl.when(jnp.logical_not(is_owner))
    def _():
        arrived(owners * piece, e_recv)

    high, low = split2(jnp.concatenate([gather3[q] for q in range(group // 2)], axis=0))
    incoming = jnp.concatenate([high, low], axis=0)
    sums = jnp.zeros((BLOCK, LANES), F32)
    place = lax.broadcasted_iota(jnp.int32, (BLOCK, LANES), 1)
    for k in range(blocks):
        rows = slice(BLOCK * k, BLOCK * (k + 1))
        read = dot(c2_s[rows, :], incoming)
        gated = base_s[rows, :] + slope_s[rows, :] * read
        base_s[rows, :] = gated
        square = gated * gated
        partial = square[:, :LANES]
        for t in range(1, tiles):
            partial = partial + square[:, LANES * t : LANES * (t + 1)]
        sums = jnp.where(place == k, jnp.sum(partial, axis=1, keepdims=True), sums)
    squares_s[...] = jnp.transpose(sums)[:blocks, :]

    def copy_f(z):
        return pltpu.make_async_remote_copy(
            squares_s, gather_sq.at[me_z], send_sem, f_recv,
            device_id=(me, z), device_id_type=MESH,
        )

    for z in range(nchan):

        @pl.when(z < me_z)
        def _():
            copy_f(z).start()

    @pl.when(me_z < nchan - 1)
    def _():
        pl.semaphore_wait(z_in, nchan - 1 - me_z)

    for z in range(nchan):

        @pl.when(z > me_z)
        def _():
            copy_f(z).start()

    gather_sq[me_z] = squares_s[...]
    for k in range(blocks):
        rows = slice(BLOCK * k, BLOCK * (k + 1))
        base_s[rows, :] = base_s[rows, :] * gain_s[...]

    arrived((nchan - 1) * blocks, f_recv)

    total = gather_sq[0]
    for z in range(1, nchan):
        total = total + gather_sq[z]
    total_ref[...] = total

    for n in range(rows_y):

        @pl.when(is_owner & (me_y == rows_y - 1 - n))
        def _():
            sent((owners - 1 + n) * (piece + 1) + (group - 1) * piece + (nchan - 1) * blocks)

    @pl.when(jnp.logical_not(is_owner))
    def _():
        sent(owners * (piece + 1) + (nchan - 1) * blocks)


def scale_rows(width, base_ref, total_ref, out_hbm, out_s, store_sem):
    tokens, channels = base_ref.shape
    blocks = tokens // BLOCK
    factor = lax.rsqrt(total_ref[...] / width + EPSILON)
    for k in range(blocks):
        for r in range(BLOCK // LANES):
            part = slice(LANES * r, LANES * (r + 1))
            rows = slice(BLOCK * k + LANES * r, BLOCK * k + LANES * (r + 1))
            scale = jnp.transpose(jnp.broadcast_to(factor[k : k + 1, part], (LANES, LANES)))
            for t in range(channels // LANES):
                lanes = slice(LANES * t, LANES * (t + 1))
                out_s[rows, lanes] = (base_ref[rows, lanes] * scale).astype(BF16)
        rows = slice(BLOCK * k, BLOCK * (k + 1))
        pltpu.make_async_copy(out_s.at[rows, :], out_hbm.at[rows, :], store_sem).start()
    pltpu.make_async_copy(out_s, out_hbm, store_sem).wait()


def per_device(group, rows_y, nchan, x, gate, b, c, step, keep, skip, gain):
    tokens, channels = x.shape
    nstate = b.shape[1]
    heads = step.shape[0]
    blocks = tokens // BLOCK
    owners = group // 2
    piece = nstate // owners
    vmem = pltpu.VMEM
    dma = pltpu.SemaphoreType.DMA
    anywhere = pl.BlockSpec(memory_space=pl.ANY)
    operands = (x, gate, b.T, c.T, step, keep, skip.reshape(1, heads), gain.reshape(1, channels))
    scratch = [
        vmem((tokens, channels), BF16), vmem((tokens, channels), BF16),
        vmem((nstate, tokens), BF16), vmem((nstate, tokens), BF16),
        vmem((2, heads, tokens), F32),
        pltpu.SMEM((1, heads), F32), vmem((1, channels), F32),
        vmem((8 * blocks, BLOCK), F32), vmem((8 * blocks, BLOCK), F32),
        vmem((8 * blocks, BLOCK), F32), vmem((8 * blocks, BLOCK), F32),
        vmem((tokens, 2 * nstate), BF16),
        vmem((blocks, channels), F32), vmem((1, channels), F32),
        vmem((blocks, nstate, channels), F32), vmem((blocks, nstate, channels), F32),
        vmem((blocks, channels), F32),
        vmem((owners, piece, channels), F32), vmem((group, piece, channels), F32),
        vmem((group, 1, channels), F32), vmem((group, piece, channels), F32),
        vmem((piece, channels), F32), vmem((1, channels), F32),
        vmem((rows_y, piece, channels), F32), vmem((rows_y, 1, channels), F32),
        vmem((piece, channels), F32),
        vmem((group, piece, channels), F32), vmem((owners, piece, channels), F32),
        vmem((tokens, channels), F32),
        vmem((blocks, BLOCK), F32), vmem((nchan, blocks, BLOCK), F32),
        vmem(((owners + rows_y) * (piece + 1) + group * piece + nchan * blocks, 1, channels), F32),
        dma((5,)), dma, dma, pltpu.SemaphoreType.REGULAR((rows_y,)), pltpu.SemaphoreType.REGULAR,
    ] + [dma] * 5
    base, total = pl.pallas_call(
        functools.partial(layer, group, rows_y, nchan),
        out_shape=(
            jax.ShapeDtypeStruct((tokens, channels), F32),
            jax.ShapeDtypeStruct((blocks, BLOCK), F32),
        ),
        in_specs=[anywhere] * 8,
        out_specs=(pl.BlockSpec(memory_space=pltpu.VMEM),) * 2,
        scratch_shapes=scratch,
        compiler_params=pltpu.CompilerParams(
            collective_id=0, has_side_effects=True, vmem_limit_bytes=24 * 1024 * 1024
        ),
    )(*[pltpu.with_memory_space_constraint(v, pltpu.HBM) for v in operands])
    return pl.pallas_call(
        functools.partial(scale_rows, channels * nchan),
        out_shape=jax.ShapeDtypeStruct((tokens, channels), BF16),
        in_specs=[pl.BlockSpec(memory_space=pltpu.VMEM)] * 2,
        out_specs=anywhere,
        scratch_shapes=[vmem((tokens, channels), BF16), dma],
        compiler_params=pltpu.CompilerParams(vmem_limit_bytes=8 * 1024 * 1024),
    )(base, total)


def build(mesh, group):
    rows_y = mesh.shape["seq"] // group
    placed = (
        P("seq", "chan"), P("seq", "chan"), P("seq", None), P("seq", None),
        P("chan", "seq"), P("chan", "seq"), P("chan"), P("chan"),
    )
    return jax.shard_map(
        functools.partial(per_device, group, rows_y, mesh.shape["chan"]),
        mesh=mesh, in_specs=placed, out_specs=P("seq", "chan"), check_vma=False,
    )


def solution(mesh):
    return build(mesh, GROUP)
```

```python
import functools

import jax
import jax.numpy as jnp
from jax import lax
from jax.experimental import pallas as pl
from jax.experimental.pallas import tpu as pltpu
from jax.sharding import PartitionSpec as P

BLOCK = 256
LANES = 128
EPSILON = 1e-05
GROUP = 8
MESH = pl.DeviceIdType.MESH
F32 = jnp.float32
BF16 = jnp.bfloat16


def split2(v):
    high = v.astype(BF16)
    return high, (v - high.astype(F32)).astype(BF16)


def dot(a, b, contract=((1,), (0,))):
    return lax.dot_general(a, b, (contract, ((), ())), preferred_element_type=F32)


def layer(
    group, rows_y, nchan,
    x_hbm, gate_hbm, b_hbm, c_hbm, step_hbm, keep_hbm, skip_hbm, gain_hbm,
    base_s, total_ref,
    x_s, gate_s, b_s, c_s, keep_step, skip_s, gain_s,
    keep8, step8, coef8, cum8, c2_s,
    totals, device_total, block_state, starts, prefix_s,
    end_s, gather1, totals1, group_prefix, group_total_state, group_total,
    gather2, totals2, entering_s, decay_s, back_s, gather3,
    slope_s, squares_s, gather_sq, lines_s,
    load_sem, keep_sem, skip_sem, y_in, z_in,
    send_sem, b_recv, d_recv, e_recv, f_recv,
):
    tokens, channels = x_s.shape
    nstate = b_s.shape[0]
    heads = keep_step.shape[1]
    width = channels // heads
    blocks = tokens // BLOCK
    tiles = channels // LANES
    per_tile = heads // tiles
    piece = 2 * nstate // group

    me = lax.axis_index("seq")
    me_z = lax.axis_index("chan")
    me_y = me // group
    me_j = me % group
    is_owner = me_j % 2 == 1
    me_q = me_j // 2

    def owner(q):
        return 2 * q + 1

    def at_group(j):
        return (me_y * group + j, me_z)

    def at_y(y):
        return (y * group + me_j, me_z)

    def lines_of(count, semaphore):
        ref = lines_s.at[pl.ds(0, count)]
        return pltpu.make_async_remote_copy(
            ref, ref, semaphore, semaphore,
            device_id=(me, (me_z + 1) % nchan), device_id_type=MESH,
        )

    def arrived(count, semaphore):
        lines_of(count, semaphore).wait_recv()

    def sent(count):
        lines_of(count, send_sem).wait_send()

    owners = group // 2

    def rank(y):
        return jnp.minimum(y, rows_y - y) * rows_y + y

    by_rank = sorted(range(rows_y), key=lambda y: min(y, rows_y - y) * rows_y + y)

    first = [
        pltpu.make_async_copy(keep_hbm, keep_step.at[0], keep_sem),
        pltpu.make_async_copy(step_hbm, keep_step.at[1], keep_sem),
        pltpu.make_async_copy(b_hbm, b_s, load_sem.at[0]),
        pltpu.make_async_copy(x_hbm, x_s, load_sem.at[1]),
    ]
    second = [
        pltpu.make_async_copy(c_hbm, c_s, load_sem.at[2]),
        pltpu.make_async_copy(gate_hbm, gate_s, load_sem.at[3]),
        pltpu.make_async_copy(gain_hbm, gain_s, load_sem.at[4]),
        pltpu.make_async_copy(skip_hbm, skip_s, skip_sem),
    ]
    for copy in first:
        copy.start()

    barrier = pltpu.get_barrier_semaphore()

    def greet(device):
        pl.semaphore_signal(barrier, inc=1, device_id=device, device_id_type=MESH)

    def report(semaphore, device):
        pl.semaphore_signal(semaphore, inc=1, device_id=device, device_id_type=MESH)

    for j in range(group):

        @pl.when((j != me_j) & is_owner)
        def _():
            greet(at_group(j))

    for y in range(rows_y):

        @pl.when(is_owner & (rank(me_y) < rank(y)))
        def _():
            greet(at_y(y))

    for z in range(nchan):

        @pl.when(me_z < z)
        def _():
            greet((me, z))

    lane = lax.broadcasted_iota(jnp.int32, (8, channels), 1)
    row8 = lax.broadcasted_iota(jnp.int32, (8, channels), 0)
    own_head = (lane // width) == row8
    half = lax.broadcasted_iota(jnp.int32, (1, LANES), 1) < width
    past = lax.broadcasted_iota(jnp.int32, (BLOCK, BLOCK), 0)
    here = lax.broadcasted_iota(jnp.int32, (BLOCK, BLOCK), 1)
    upper = jnp.where(past <= here, 1.0, 0.0).astype(BF16)
    later = jnp.where(past > here, 1.0, 0.0).astype(BF16)

    pltpu.make_async_copy(keep_step, keep_step, keep_sem).wait()
    for copy in second:
        copy.start()
    keep8[...] = jnp.zeros_like(keep8)
    step8[...] = jnp.zeros_like(step8)
    for k in range(blocks):
        keep8[8 * k : 8 * k + heads, :] = keep_step[0, :, BLOCK * k : BLOCK * (k + 1)]
        step8[8 * k : 8 * k + heads, :] = keep_step[1, :, BLOCK * k : BLOCK * (k + 1)]
    keep = keep8[...]
    k_high = keep.astype(BF16)
    k_mid, k_low = split2(keep - k_high.astype(F32))
    after = dot(k_high, later) + (dot(k_mid, later) + dot(k_low, later))
    coef8[...] = jnp.exp(after) * step8[...]

    first[2].wait()
    first[3].wait()
    cum8[...] = dot(k_high, upper) + (dot(k_mid, upper) + dot(k_low, upper))
    for k in range(blocks):
        coef = coef8[8 * k : 8 * k + 8, :]
        bt = b_s[:, BLOCK * k : BLOCK * (k + 1)].astype(F32)
        for t in range(tiles):
            lines = jnp.concatenate(
                [(bt * coef[h : h + 1, :]).astype(BF16) for h in (2 * t, 2 * t + 1)], axis=0
            )
            both = dot(lines, x_s[BLOCK * k : BLOCK * (k + 1), LANES * t : LANES * (t + 1)])
            block_state[k, :, LANES * t : LANES * (t + 1)] = jnp.where(
                half, both[:nstate], both[nstate:]
            )
    for k in range(blocks):
        last = cum8[8 * k : 8 * k + 8, BLOCK - 1 : BLOCK]
        spread = jnp.where(own_head, jnp.broadcast_to(last, (8, channels)), 0.0)
        totals[k : k + 1, :] = jnp.sum(spread, axis=0, keepdims=True)
    device_total[...] = jnp.sum(totals[...], axis=0, keepdims=True)
    running = jnp.zeros((nstate, channels), F32)
    for k in range(blocks):
        starts[k] = running
        running = jnp.exp(totals[k : k + 1, :]) * running + block_state[k]
    for q in range(group // 2):
        end_s[q] = running[piece * q : piece * (q + 1), :]

    greeted = me_z + jnp.where(is_owner, owners - 1, owners)
    for y in range(rows_y):
        greeted = greeted + jnp.where(is_owner & (rank(y) < rank(me_y)), 1, 0)
    pl.semaphore_wait(barrier, greeted)

    def copy_a(i):
        return pltpu.make_async_remote_copy(
            device_total, totals1.at[me_j], send_sem, b_recv,
            device_id=at_group(owner((me_q + i) % (group // 2))), device_id_type=MESH,
        )

    def copy_b(i):
        q = (me_q + i) % (group // 2)
        return pltpu.make_async_remote_copy(
            end_s.at[q], gather1.at[me_j], send_sem, b_recv,
            device_id=at_group(owner(q)), device_id_type=MESH,
        )

    others = [group // 4] + [i for i in range(group // 2) if i != group // 4]
    for i in others:

        @pl.when((i != 0) | jnp.logical_not(is_owner))
        def _():
            copy_a(i).start()
            copy_b(i).start()

    for y in range(rows_y):

        @pl.when(is_owner & (y < me_y) & (rank(y) < rank(me_y)))
        def _():
            report(y_in.at[me_y], at_y(y))

    for z in range(nchan):

        @pl.when(z < me_z)
        def _():
            report(z_in, (me, z))

    @pl.when(is_owner)
    def _():
        gather1[me_j] = end_s[me_q]
        totals1[me_j] = device_total[...]

    before = jnp.zeros((1, channels), F32)
    for k in range(blocks):
        prefix_s[k : k + 1, :] = before
        before = before + totals[k : k + 1, :]

    for copy in second:
        copy.wait()
    head_of = lax.broadcasted_iota(jnp.int32, (1, channels), 1) // width
    skip_row = jnp.zeros((1, channels), F32)
    for h in range(heads):
        skip_row = jnp.where(head_of == h, skip_s[0, h], skip_row)
    diagonal = (
        lax.broadcasted_iota(jnp.int32, (LANES, LANES), 0)
        >= lax.broadcasted_iota(jnp.int32, (LANES, LANES), 1)
    )

    def inside(k, carry):
        rows = pl.ds(pl.multiple_of(k * BLOCK, BLOCK), BLOCK)
        slab_at = pl.ds(pl.multiple_of(k * 8, 8), 8)
        slab = cum8[slab_at, :]
        steps = step8[slab_at, :]
        columns = jnp.transpose(slab)
        c_block = c_s[:, rows]
        c_pair = jnp.transpose(jnp.concatenate([c_block, c_block], axis=0))
        c2_s[rows, :] = c_pair
        scores = dot(c_pair[:, :nstate], b_s[:, rows])
        high, low = split2(starts[k])
        read = dot(c_pair, jnp.concatenate([high, low], axis=0))
        carried = jnp.exp(prefix_s[pl.ds(k, 1), :])
        for t in range(tiles):
            lanes = slice(LANES * t, LANES * (t + 1))
            weights, spreads = [], []
            for h in (2 * t, 2 * t + 1):
                column = jnp.broadcast_to(columns[:, h : h + 1], (BLOCK, LANES))
                spreads.append(column)

                def weight(r, s):
                    rr, ss = slice(LANES * r, LANES * (r + 1)), slice(LANES * s, LANES * (s + 1))
                    w = (
                        scores[rr, ss]
                        * jnp.exp(column[rr, :] - slab[h : h + 1, ss])
                        * steps[h : h + 1, ss]
                    )
                    return (jnp.where(diagonal, w, 0.0) if r == s else w).astype(BF16)

                top = jnp.concatenate([weight(0, 0), jnp.zeros((LANES, LANES), BF16)], axis=1)
                bottom = jnp.concatenate([weight(1, 0), weight(1, 1)], axis=1)
                weights += [top, bottom]
            x_tile = x_s[rows, lanes]
            both = dot(jnp.concatenate(weights, axis=0), x_tile)
            value = jnp.where(half, both[:BLOCK], both[BLOCK:])
            value = value + skip_row[:, lanes] * x_tile.astype(F32)
            gate = gate_s[rows, lanes].astype(F32)
            gate = gate / (1.0 + jnp.exp(-gate))
            slope = jnp.exp(jnp.where(half, spreads[0], spreads[1])) * gate
            base_s[rows, lanes] = value * gate + slope * read[:, lanes]
            slope_s[rows, lanes] = slope * carried[:, lanes]
        return carry

    third = (blocks * 3) // 8
    middle = jnp.where(me_y > 0, third + blocks // 4, third)
    lax.fori_loop(0, third, inside, 0)

    def copy_c(y):
        return pltpu.make_async_remote_copy(
            group_total, totals2.at[me_y], send_sem, d_recv,
            device_id=at_y(y), device_id_type=MESH,
        )

    def copy_d(y):
        return pltpu.make_async_remote_copy(
            group_total_state, gather2.at[me_y], send_sem, d_recv,
            device_id=at_y(y), device_id_type=MESH,
        )

    @pl.when(is_owner)
    def _():
        arrived((group - 1) * (piece + 1), b_recv)
        total = totals1[0]
        for m in range(1, group):
            total = total + totals1[m]
        group_total[...] = total
        state = jnp.zeros((piece, channels), F32)
        for m in range(group):
            group_prefix[m] = state
            state = jnp.exp(totals1[m]) * state + gather1[m]
        group_total_state[...] = state
        for y in by_rank:

            @pl.when((y > me_y) & (rank(me_y) < rank(y)))
            def _():
                pl.semaphore_wait(y_in.at[y], 1)

            @pl.when(y > me_y)
            def _():
                copy_c(y).start()
                copy_d(y).start()

    def copy_e(i):
        p = (me_j + i) % group
        return pltpu.make_async_remote_copy(
            back_s.at[p], gather3.at[me_q], send_sem, e_recv,
            device_id=at_group(p), device_id_type=MESH,
        )

    @pl.when(is_owner)
    def _():
        ahead = jnp.zeros((1, channels), F32)
        for m in range(group):
            decay_s[m] = jnp.exp(ahead)
            ahead = ahead + totals1[m]

    lax.fori_loop(third, middle, inside, 0)

    @pl.when(is_owner)
    def _():
        entering_s[...] = jnp.zeros_like(entering_s)
        for n in range(1, rows_y):

            @pl.when(me_y == n)
            def _():
                arrived(n * (piece + 1), d_recv)
                state = gather2[0]
                for y in range(1, n):
                    state = jnp.exp(totals2[y]) * state + gather2[y]
                entering_s[...] = state

        entering = entering_s[...]
        for i in sorted(range(1, group), key=lambda i: i % 2 - 2 * min((i + 1) // 2, (group - i) // 2) - 3 * (i % 2)):
            p = (me_j + i) % group
            back_s[p] = decay_s[p] * entering + group_prefix[p]
            copy_e(i).start()
        back_s[me_j] = decay_s[me_j] * entering + group_prefix[me_j]
        gather3[me_q] = back_s[me_j]

    lax.fori_loop(middle, blocks, inside, 0)

    @pl.when(is_owner)
    def _():
        arrived((owners - 1) * piece, e_recv)

    @pl.when(jnp.logical_not(is_owner))
    def _():
        arrived(owners * piece, e_recv)

    high, low = split2(jnp.concatenate([gather3[q] for q in range(group // 2)], axis=0))
    incoming = jnp.concatenate([high, low], axis=0)
    sums = jnp.zeros((BLOCK, LANES), F32)
    place = lax.broadcasted_iota(jnp.int32, (BLOCK, LANES), 1)
    for k in range(blocks):
        rows = slice(BLOCK * k, BLOCK * (k + 1))
        read = dot(c2_s[rows, :], incoming)
        gated = base_s[rows, :] + slope_s[rows, :] * read
        base_s[rows, :] = gated
        square = gated * gated
        partial = square[:, :LANES]
        for t in range(1, tiles):
            partial = partial + square[:, LANES * t : LANES * (t + 1)]
        sums = jnp.where(place == k, jnp.sum(partial, axis=1, keepdims=True), sums)
    squares_s[...] = jnp.transpose(sums)[:blocks, :]

    def copy_f(z):
        return pltpu.make_async_remote_copy(
            squares_s, gather_sq.at[me_z], send_sem, f_recv,
            device_id=(me, z), device_id_type=MESH,
        )

    for z in range(nchan):

        @pl.when(z < me_z)
        def _():
            copy_f(z).start()

    @pl.when(me_z < nchan - 1)
    def _():
        pl.semaphore_wait(z_in, nchan - 1 - me_z)

    for z in range(nchan):

        @pl.when(z > me_z)
        def _():
            copy_f(z).start()

    gather_sq[me_z] = squares_s[...]
    for k in range(blocks):
        rows = slice(BLOCK * k, BLOCK * (k + 1))
        base_s[rows, :] = base_s[rows, :] * gain_s[...]

    arrived((nchan - 1) * blocks, f_recv)

    total = gather_sq[0]
    for z in range(1, nchan):
        total = total + gather_sq[z]
    total_ref[...] = total

    for n in range(rows_y):

        @pl.when(is_owner & (me_y == rows_y - 1 - n))
        def _():
            sent((owners - 1 + n) * (piece + 1) + (group - 1) * piece + (nchan - 1) * blocks)

    @pl.when(jnp.logical_not(is_owner))
    def _():
        sent(owners * (piece + 1) + (nchan - 1) * blocks)


def scale_rows(width, base_ref, total_ref, out_hbm, out_s, store_sem):
    tokens, channels = base_ref.shape
    blocks = tokens // BLOCK
    factor = lax.rsqrt(total_ref[...] / width + EPSILON)
    for k in range(blocks):
        for r in range(BLOCK // LANES):
            part = slice(LANES * r, LANES * (r + 1))
            rows = slice(BLOCK * k + LANES * r, BLOCK * k + LANES * (r + 1))
            scale = jnp.transpose(jnp.broadcast_to(factor[k : k + 1, part], (LANES, LANES)))
            for t in range(channels // LANES):
                lanes = slice(LANES * t, LANES * (t + 1))
                out_s[rows, lanes] = (base_ref[rows, lanes] * scale).astype(BF16)
        rows = slice(BLOCK * k, BLOCK * (k + 1))
        pltpu.make_async_copy(out_s.at[rows, :], out_hbm.at[rows, :], store_sem).start()
    pltpu.make_async_copy(out_s, out_hbm, store_sem).wait()


def per_device(group, rows_y, nchan, x, gate, b, c, step, keep, skip, gain):
    tokens, channels = x.shape
    nstate = b.shape[1]
    heads = step.shape[0]
    blocks = tokens // BLOCK
    owners = group // 2
    piece = nstate // owners
    vmem = pltpu.VMEM
    dma = pltpu.SemaphoreType.DMA
    anywhere = pl.BlockSpec(memory_space=pl.ANY)
    operands = (x, gate, b.T, c.T, step, keep, skip.reshape(1, heads), gain.reshape(1, channels))
    scratch = [
        vmem((tokens, channels), BF16), vmem((tokens, channels), BF16),
        vmem((nstate, tokens), BF16), vmem((nstate, tokens), BF16),
        vmem((2, heads, tokens), F32),
        pltpu.SMEM((1, heads), F32), vmem((1, channels), F32),
        vmem((8 * blocks, BLOCK), F32), vmem((8 * blocks, BLOCK), F32),
        vmem((8 * blocks, BLOCK), F32), vmem((8 * blocks, BLOCK), F32),
        vmem((tokens, 2 * nstate), BF16),
        vmem((blocks, channels), F32), vmem((1, channels), F32),
        vmem((blocks, nstate, channels), F32), vmem((blocks, nstate, channels), F32),
        vmem((blocks, channels), F32),
        vmem((owners, piece, channels), F32), vmem((group, piece, channels), F32),
        vmem((group, 1, channels), F32), vmem((group, piece, channels), F32),
        vmem((piece, channels), F32), vmem((1, channels), F32),
        vmem((rows_y, piece, channels), F32), vmem((rows_y, 1, channels), F32),
        vmem((piece, channels), F32), vmem((group, 1, channels), F32),
        vmem((group, piece, channels), F32), vmem((owners, piece, channels), F32),
        vmem((tokens, channels), F32),
        vmem((blocks, BLOCK), F32), vmem((nchan, blocks, BLOCK), F32),
        vmem(((owners + rows_y) * (piece + 1) + group * piece + nchan * blocks, 1, channels), F32),
        dma((5,)), dma, dma, pltpu.SemaphoreType.REGULAR((rows_y,)), pltpu.SemaphoreType.REGULAR,
    ] + [dma] * 5
    base, total = pl.pallas_call(
        functools.partial(layer, group, rows_y, nchan),
        out_shape=(
            jax.ShapeDtypeStruct((tokens, channels), F32),
            jax.ShapeDtypeStruct((blocks, BLOCK), F32),
        ),
        in_specs=[anywhere] * 8,
        out_specs=(pl.BlockSpec(memory_space=pltpu.VMEM),) * 2,
        scratch_shapes=scratch,
        compiler_params=pltpu.CompilerParams(
            collective_id=0, has_side_effects=True, vmem_limit_bytes=24 * 1024 * 1024
        ),
    )(*[pltpu.with_memory_space_constraint(v, pltpu.HBM) for v in operands])
    return pl.pallas_call(
        functools.partial(scale_rows, channels * nchan),
        out_shape=jax.ShapeDtypeStruct((tokens, channels), BF16),
        in_specs=[pl.BlockSpec(memory_space=pltpu.VMEM)] * 2,
        out_specs=anywhere,
        scratch_shapes=[vmem((tokens, channels), BF16), dma],
        compiler_params=pltpu.CompilerParams(vmem_limit_bytes=8 * 1024 * 1024),
    )(base, total)


def build(mesh, group):
    rows_y = mesh.shape["seq"] // group
    placed = (
        P("seq", "chan"), P("seq", "chan"), P("seq", None), P("seq", None),
        P("chan", "seq"), P("chan", "seq"), P("chan"), P("chan"),
    )
    return jax.shard_map(
        functools.partial(per_device, group, rows_y, mesh.shape["chan"]),
        mesh=mesh, in_specs=placed, out_specs=P("seq", "chan"), check_vma=False,
    )


def solution(mesh):
    return build(mesh, GROUP)
```

```python
import functools

import jax
import jax.numpy as jnp
from jax import lax
from jax.experimental import pallas as pl
from jax.experimental.pallas import tpu as pltpu
from jax.sharding import PartitionSpec as P

BLOCK = 256
LANES = 128
EPSILON = 1e-05
GROUP = 8
MESH = pl.DeviceIdType.MESH
F32 = jnp.float32
BF16 = jnp.bfloat16


def split2(v):
    high = v.astype(BF16)
    return high, (v - high.astype(F32)).astype(BF16)


def dot(a, b, contract=((1,), (0,))):
    return lax.dot_general(a, b, (contract, ((), ())), preferred_element_type=F32)


def layer(
    group, rows_y, nchan,
    x_hbm, gate_hbm, b_hbm, c_hbm, step_hbm, keep_hbm, skip_hbm, gain_hbm,
    base_s, total_ref,
    x_s, gate_s, b_s, c_s, keep_step, skip_s, gain_s,
    keep8, step8, coef8, cum8, c2_s,
    totals, device_total, block_state, starts, prefix_s,
    end_s, gather1, totals1, group_prefix, group_total_state, group_total,
    gather2, totals2, entering_s, decay_s, back_s, gather3,
    slope_s, squares_s, gather_sq, lines_s,
    load_sem, keep_sem, skip_sem, y_in, z_in,
    send_sem, b_recv, d_recv, e_recv, f_recv,
):
    tokens, channels = x_s.shape
    nstate = b_s.shape[0]
    heads = keep_step.shape[1]
    width = channels // heads
    blocks = tokens // BLOCK
    tiles = channels // LANES
    per_tile = heads // tiles
    piece = 2 * nstate // group

    me = lax.axis_index("seq")
    me_z = lax.axis_index("chan")
    me_y = me // group
    me_j = me % group
    is_owner = me_j % 2 == 1
    me_q = me_j // 2

    def owner(q):
        return 2 * q + 1

    def at_group(j):
        return (me_y * group + j, me_z)

    def at_y(y):
        return (y * group + me_j, me_z)

    def lines_of(count, semaphore):
        ref = lines_s.at[pl.ds(0, count)]
        return pltpu.make_async_remote_copy(
            ref, ref, semaphore, semaphore,
            device_id=(me, (me_z + 1) % nchan), device_id_type=MESH,
        )

    def arrived(count, semaphore):
        lines_of(count, semaphore).wait_recv()

    def sent(count):
        lines_of(count, send_sem).wait_send()

    owners = group // 2
    both_lines = nstate * tokens // (2 * channels) + tokens // 2

    def loaded(count, i):
        ref = lines_s.at[pl.ds(0, count)]
        pltpu.make_async_copy(ref, ref, load_sem.at[i]).wait()

    def rank(y):
        return jnp.minimum(y, rows_y - y) * rows_y + y

    by_rank = sorted(range(rows_y), key=lambda y: min(y, rows_y - y) * rows_y + y)

    first = [
        pltpu.make_async_copy(keep_hbm, keep_step.at[0], keep_sem),
        pltpu.make_async_copy(step_hbm, keep_step.at[1], keep_sem),
        pltpu.make_async_copy(b_hbm, b_s, load_sem.at[0]),
    ]
    parts = [
        pltpu.make_async_copy(x_hbm.at[part, :], x_s.at[part, :], load_sem.at[0])
        for part in (pl.ds(i * (tokens // 4), tokens // 4) for i in range(4))
    ]
    second = [
        pltpu.make_async_copy(c_hbm, c_s, load_sem.at[1]),
        pltpu.make_async_copy(gate_hbm, gate_s, load_sem.at[1]),
        pltpu.make_async_copy(gain_hbm, gain_s, load_sem.at[1]),
        pltpu.make_async_copy(skip_hbm, skip_s, skip_sem),
    ]
    for copy in first:
        copy.start()
    for copy in parts:
        copy.start(priority=1)

    barrier = pltpu.get_barrier_semaphore()

    def greet(device):
        pl.semaphore_signal(barrier, inc=1, device_id=device, device_id_type=MESH)

    def report(semaphore, device):
        pl.semaphore_signal(semaphore, inc=1, device_id=device, device_id_type=MESH)

    for j in range(group):

        @pl.when((j != me_j) & is_owner)
        def _():
            greet(at_group(j))

    for y in range(rows_y):

        @pl.when(is_owner & (rank(me_y) < rank(y)))
        def _():
            greet(at_y(y))

    for z in range(nchan):

        @pl.when(me_z < z)
        def _():
            greet((me, z))

    lane = lax.broadcasted_iota(jnp.int32, (8, channels), 1)
    row8 = lax.broadcasted_iota(jnp.int32, (8, channels), 0)
    own_head = (lane // width) == row8
    half = lax.broadcasted_iota(jnp.int32, (1, LANES), 1) < width
    past = lax.broadcasted_iota(jnp.int32, (BLOCK, BLOCK), 0)
    here = lax.broadcasted_iota(jnp.int32, (BLOCK, BLOCK), 1)
    upper = jnp.where(past <= here, 1.0, 0.0).astype(BF16)
    later = jnp.where(past > here, 1.0, 0.0).astype(BF16)

    pltpu.make_async_copy(keep_step, keep_step, keep_sem).wait()
    for copy in second:
        copy.start()
    keep8[...] = jnp.zeros_like(keep8)
    step8[...] = jnp.zeros_like(step8)
    for k in range(blocks):
        keep8[8 * k : 8 * k + heads, :] = keep_step[0, :, BLOCK * k : BLOCK * (k + 1)]
        step8[8 * k : 8 * k + heads, :] = keep_step[1, :, BLOCK * k : BLOCK * (k + 1)]
    keep = keep8[...]
    k_high = keep.astype(BF16)
    k_mid, k_low = split2(keep - k_high.astype(F32))
    after = dot(k_high, later) + (dot(k_mid, later) + dot(k_low, later))
    coef8[...] = jnp.exp(after) * step8[...]

    loaded(both_lines, 0)
    cum8[...] = dot(k_high, upper) + (dot(k_mid, upper) + dot(k_low, upper))
    for k in range(blocks):
        coef = coef8[8 * k : 8 * k + 8, :]
        bt = b_s[:, BLOCK * k : BLOCK * (k + 1)].astype(F32)
        for t in range(tiles):
            lines = jnp.concatenate(
                [(bt * coef[h : h + 1, :]).astype(BF16) for h in (2 * t, 2 * t + 1)], axis=0
            )
            both = dot(lines, x_s[BLOCK * k : BLOCK * (k + 1), LANES * t : LANES * (t + 1)])
            block_state[k, :, LANES * t : LANES * (t + 1)] = jnp.where(
                half, both[:nstate], both[nstate:]
            )
    for k in range(blocks):
        last = cum8[8 * k : 8 * k + 8, BLOCK - 1 : BLOCK]
        spread = jnp.where(own_head, jnp.broadcast_to(last, (8, channels)), 0.0)
        totals[k : k + 1, :] = jnp.sum(spread, axis=0, keepdims=True)
    device_total[...] = jnp.sum(totals[...], axis=0, keepdims=True)
    running = jnp.zeros((nstate, channels), F32)
    for k in range(blocks):
        starts[k] = running
        running = jnp.exp(totals[k : k + 1, :]) * running + block_state[k]
    for q in range(group // 2):
        end_s[q] = running[piece * q : piece * (q + 1), :]

    greeted = me_z + jnp.where(is_owner, owners - 1, owners)
    for y in range(rows_y):
        greeted = greeted + jnp.where(is_owner & (rank(y) < rank(me_y)), 1, 0)
    pl.semaphore_wait(barrier, greeted)

    def copy_a(i):
        return pltpu.make_async_remote_copy(
            device_total, totals1.at[me_j], send_sem, b_recv,
            device_id=at_group(owner((me_q + i) % (group // 2))), device_id_type=MESH,
        )

    def copy_b(i):
        q = (me_q + i) % (group // 2)
        return pltpu.make_async_remote_copy(
            end_s.at[q], gather1.at[me_j], send_sem, b_recv,
            device_id=at_group(owner(q)), device_id_type=MESH,
        )

    others = [group // 4] + [i for i in range(group // 2) if i != group // 4]
    for i in others:

        @pl.when((i != 0) | jnp.logical_not(is_owner))
        def _():
            copy_a(i).start()
            copy_b(i).start()

    for y in range(rows_y):

        @pl.when(is_owner & (y < me_y) & (rank(y) < rank(me_y)))
        def _():
            report(y_in.at[me_y], at_y(y))

    for z in range(nchan):

        @pl.when(z < me_z)
        def _():
            report(z_in, (me, z))

    @pl.when(is_owner)
    def _():
        gather1[me_j] = end_s[me_q]
        totals1[me_j] = device_total[...]

    before = jnp.zeros((1, channels), F32)
    for k in range(blocks):
        prefix_s[k : k + 1, :] = before
        before = before + totals[k : k + 1, :]

    loaded(both_lines + 1, 1)
    second[-1].wait()
    head_of = lax.broadcasted_iota(jnp.int32, (1, channels), 1) // width
    skip_row = jnp.zeros((1, channels), F32)
    for h in range(heads):
        skip_row = jnp.where(head_of == h, skip_s[0, h], skip_row)
    diagonal = (
        lax.broadcasted_iota(jnp.int32, (LANES, LANES), 0)
        >= lax.broadcasted_iota(jnp.int32, (LANES, LANES), 1)
    )

    def inside(k, carry):
        rows = pl.ds(pl.multiple_of(k * BLOCK, BLOCK), BLOCK)
        slab_at = pl.ds(pl.multiple_of(k * 8, 8), 8)
        slab = cum8[slab_at, :]
        steps = step8[slab_at, :]
        columns = jnp.transpose(slab)
        c_block = c_s[:, rows]
        c_pair = jnp.transpose(jnp.concatenate([c_block, c_block], axis=0))
        c2_s[rows, :] = c_pair
        scores = dot(c_pair[:, :nstate], b_s[:, rows])
        high, low = split2(starts[k])
        read = dot(c_pair, jnp.concatenate([high, low], axis=0))
        carried = jnp.exp(prefix_s[pl.ds(k, 1), :])
        for t in range(tiles):
            lanes = slice(LANES * t, LANES * (t + 1))
            weights, spreads = [], []
            for h in (2 * t, 2 * t + 1):
                column = jnp.broadcast_to(columns[:, h : h + 1], (BLOCK, LANES))
                spreads.append(column)

                def weight(r, s):
                    rr, ss = slice(LANES * r, LANES * (r + 1)), slice(LANES * s, LANES * (s + 1))
                    w = (
                        scores[rr, ss]
                        * jnp.exp(column[rr, :] - slab[h : h + 1, ss])
                        * steps[h : h + 1, ss]
                    )
                    return (jnp.where(diagonal, w, 0.0) if r == s else w).astype(BF16)

                top = jnp.concatenate([weight(0, 0), jnp.zeros((LANES, LANES), BF16)], axis=1)
                bottom = jnp.concatenate([weight(1, 0), weight(1, 1)], axis=1)
                weights += [top, bottom]
            x_tile = x_s[rows, lanes]
            both = dot(jnp.concatenate(weights, axis=0), x_tile)
            value = jnp.where(half, both[:BLOCK], both[BLOCK:])
            value = value + skip_row[:, lanes] * x_tile.astype(F32)
            gate = gate_s[rows, lanes].astype(F32)
            gate = gate / (1.0 + jnp.exp(-gate))
            slope = jnp.exp(jnp.where(half, spreads[0], spreads[1])) * gate
            base_s[rows, lanes] = value * gate + slope * read[:, lanes]
            slope_s[rows, lanes] = slope * carried[:, lanes]
        return carry

    third = (blocks * 3) // 8
    middle = jnp.where(me_y > 0, third + blocks // 4, third)
    lax.fori_loop(0, third, inside, 0)

    def copy_c(y):
        return pltpu.make_async_remote_copy(
            group_total, totals2.at[me_y], send_sem, d_recv,
            device_id=at_y(y), device_id_type=MESH,
        )

    def copy_d(y):
        return pltpu.make_async_remote_copy(
            group_total_state, gather2.at[me_y], send_sem, d_recv,
            device_id=at_y(y), device_id_type=MESH,
        )

    @pl.when(is_owner)
    def _():
        arrived((group - 1) * (piece + 1), b_recv)
        total = totals1[0]
        for m in range(1, group):
            total = total + totals1[m]
        group_total[...] = total
        state = jnp.zeros((piece, channels), F32)
        for m in range(group):
            group_prefix[m] = state
            state = jnp.exp(totals1[m]) * state + gather1[m]
        group_total_state[...] = state
        for y in by_rank:

            @pl.when((y > me_y) & (rank(me_y) < rank(y)))
            def _():
                pl.semaphore_wait(y_in.at[y], 1)

            @pl.when(y > me_y)
            def _():
                copy_c(y).start()
                copy_d(y).start()

    def copy_e(i):
        p = (me_j + i) % group
        return pltpu.make_async_remote_copy(
            back_s.at[p], gather3.at[me_q], send_sem, e_recv,
            device_id=at_group(p), device_id_type=MESH,
        )

    @pl.when(is_owner)
    def _():
        ahead = jnp.zeros((1, channels), F32)
        for m in range(group):
            decay_s[m] = jnp.exp(ahead)
            ahead = ahead + totals1[m]

    lax.fori_loop(third, middle, inside, 0)

    @pl.when(is_owner)
    def _():
        entering_s[...] = jnp.zeros_like(entering_s)
        for n in range(1, rows_y):

            @pl.when(me_y == n)
            def _():
                arrived(n * (piece + 1), d_recv)
                state = gather2[0]
                for y in range(1, n):
                    state = jnp.exp(totals2[y]) * state + gather2[y]
                entering_s[...] = state

        entering = entering_s[...]
        for i in sorted(range(1, group), key=lambda i: i % 2 - 2 * min((i + 1) // 2, (group - i) // 2) - 3 * (i % 2)):
            p = (me_j + i) % group
            back_s[p] = decay_s[p] * entering + group_prefix[p]
            copy_e(i).start()
        back_s[me_j] = decay_s[me_j] * entering + group_prefix[me_j]
        gather3[me_q] = back_s[me_j]

    lax.fori_loop(middle, blocks, inside, 0)

    @pl.when(is_owner)
    def _():
        arrived((owners - 1) * piece, e_recv)

    @pl.when(jnp.logical_not(is_owner))
    def _():
        arrived(owners * piece, e_recv)

    high, low = split2(jnp.concatenate([gather3[q] for q in range(group // 2)], axis=0))
    incoming = jnp.concatenate([high, low], axis=0)
    sums = jnp.zeros((BLOCK, LANES), F32)
    place = lax.broadcasted_iota(jnp.int32, (BLOCK, LANES), 1)
    for k in range(blocks):
        rows = slice(BLOCK * k, BLOCK * (k + 1))
        read = dot(c2_s[rows, :], incoming)
        gated = base_s[rows, :] + slope_s[rows, :] * read
        base_s[rows, :] = gated
        square = gated * gated
        partial = square[:, :LANES]
        for t in range(1, tiles):
            partial = partial + square[:, LANES * t : LANES * (t + 1)]
        sums = jnp.where(place == k, jnp.sum(partial, axis=1, keepdims=True), sums)
    squares_s[...] = jnp.transpose(sums)[:blocks, :]

    def copy_f(z):
        return pltpu.make_async_remote_copy(
            squares_s, gather_sq.at[me_z], send_sem, f_recv,
            device_id=(me, z), device_id_type=MESH,
        )

    for z in range(nchan):

        @pl.when(z < me_z)
        def _():
            copy_f(z).start()

    @pl.when(me_z < nchan - 1)
    def _():
        pl.semaphore_wait(z_in, nchan - 1 - me_z)

    for z in range(nchan):

        @pl.when(z > me_z)
        def _():
            copy_f(z).start()

    gather_sq[me_z] = squares_s[...]
    for k in range(blocks):
        rows = slice(BLOCK * k, BLOCK * (k + 1))
        base_s[rows, :] = base_s[rows, :] * gain_s[...]

    arrived((nchan - 1) * blocks, f_recv)

    total = gather_sq[0]
    for z in range(1, nchan):
        total = total + gather_sq[z]
    total_ref[...] = total

    for n in range(rows_y):

        @pl.when(is_owner & (me_y == rows_y - 1 - n))
        def _():
            sent((owners - 1 + n) * (piece + 1) + (group - 1) * piece + (nchan - 1) * blocks)

    @pl.when(jnp.logical_not(is_owner))
    def _():
        sent(owners * (piece + 1) + (nchan - 1) * blocks)


def scale_rows(width, base_ref, total_ref, out_hbm, out_s, store_sem):
    tokens, channels = base_ref.shape
    blocks = tokens // BLOCK
    factor = lax.rsqrt(total_ref[...] / width + EPSILON)
    for k in range(blocks):
        for r in range(BLOCK // LANES):
            part = slice(LANES * r, LANES * (r + 1))
            rows = slice(BLOCK * k + LANES * r, BLOCK * k + LANES * (r + 1))
            scale = jnp.transpose(jnp.broadcast_to(factor[k : k + 1, part], (LANES, LANES)))
            for t in range(channels // LANES):
                lanes = slice(LANES * t, LANES * (t + 1))
                out_s[rows, lanes] = (base_ref[rows, lanes] * scale).astype(BF16)
        rows = slice(BLOCK * k, BLOCK * (k + 1))
        pltpu.make_async_copy(out_s.at[rows, :], out_hbm.at[rows, :], store_sem).start()
    pltpu.make_async_copy(out_s, out_hbm, store_sem).wait()


def per_device(group, rows_y, nchan, x, gate, b, c, step, keep, skip, gain):
    tokens, channels = x.shape
    nstate = b.shape[1]
    heads = step.shape[0]
    blocks = tokens // BLOCK
    owners = group // 2
    piece = nstate // owners
    vmem = pltpu.VMEM
    dma = pltpu.SemaphoreType.DMA
    anywhere = pl.BlockSpec(memory_space=pl.ANY)
    operands = (x, gate, b.T, c.T, step, keep, skip.reshape(1, heads), gain.reshape(1, channels))
    scratch = [
        vmem((tokens, channels), BF16), vmem((tokens, channels), BF16),
        vmem((nstate, tokens), BF16), vmem((nstate, tokens), BF16),
        vmem((2, heads, tokens), F32),
        pltpu.SMEM((1, heads), F32), vmem((1, channels), F32),
        vmem((8 * blocks, BLOCK), F32), vmem((8 * blocks, BLOCK), F32),
        vmem((8 * blocks, BLOCK), F32), vmem((8 * blocks, BLOCK), F32),
        vmem((tokens, 2 * nstate), BF16),
        vmem((blocks, channels), F32), vmem((1, channels), F32),
        vmem((blocks, nstate, channels), F32), vmem((blocks, nstate, channels), F32),
        vmem((blocks, channels), F32),
        vmem((owners, piece, channels), F32), vmem((group, piece, channels), F32),
        vmem((group, 1, channels), F32), vmem((group, piece, channels), F32),
        vmem((piece, channels), F32), vmem((1, channels), F32),
        vmem((rows_y, piece, channels), F32), vmem((rows_y, 1, channels), F32),
        vmem((piece, channels), F32), vmem((group, 1, channels), F32),
        vmem((group, piece, channels), F32), vmem((owners, piece, channels), F32),
        vmem((tokens, channels), F32),
        vmem((blocks, BLOCK), F32), vmem((nchan, blocks, BLOCK), F32),
        vmem((max((owners + rows_y) * (piece + 1) + group * piece + nchan * blocks, nstate * tokens // (2 * channels) + tokens // 2 + 1), 1, channels), F32),
        dma((2,)), dma, dma, pltpu.SemaphoreType.REGULAR((rows_y,)), pltpu.SemaphoreType.REGULAR,
    ] + [dma] * 5
    base, total = pl.pallas_call(
        functools.partial(layer, group, rows_y, nchan),
        out_shape=(
            jax.ShapeDtypeStruct((tokens, channels), F32),
            jax.ShapeDtypeStruct((blocks, BLOCK), F32),
        ),
        in_specs=[anywhere] * 8,
        out_specs=(pl.BlockSpec(memory_space=pltpu.VMEM),) * 2,
        scratch_shapes=scratch,
        compiler_params=pltpu.CompilerParams(
            collective_id=0, has_side_effects=True, vmem_limit_bytes=24 * 1024 * 1024
        ),
    )(*[pltpu.with_memory_space_constraint(v, pltpu.HBM) for v in operands])
    return pl.pallas_call(
        functools.partial(scale_rows, channels * nchan),
        out_shape=jax.ShapeDtypeStruct((tokens, channels), BF16),
        in_specs=[pl.BlockSpec(memory_space=pltpu.VMEM)] * 2,
        out_specs=anywhere,
        scratch_shapes=[vmem((tokens, channels), BF16), dma],
        compiler_params=pltpu.CompilerParams(vmem_limit_bytes=8 * 1024 * 1024),
    )(base, total)


def build(mesh, group):
    rows_y = mesh.shape["seq"] // group
    placed = (
        P("seq", "chan"), P("seq", "chan"), P("seq", None), P("seq", None),
        P("chan", "seq"), P("chan", "seq"), P("chan"), P("chan"),
    )
    return jax.shard_map(
        functools.partial(per_device, group, rows_y, mesh.shape["chan"]),
        mesh=mesh, in_specs=placed, out_specs=P("seq", "chan"), check_vma=False,
    )


def solution(mesh):
    return build(mesh, GROUP)
```

```python
import functools

import jax
import jax.numpy as jnp
from jax import lax
from jax.experimental import pallas as pl
from jax.experimental.pallas import tpu as pltpu
from jax.sharding import PartitionSpec as P

BLOCK = 256
LANES = 128
EPSILON = 1e-05
GROUP = 8
MESH = pl.DeviceIdType.MESH
F32 = jnp.float32
BF16 = jnp.bfloat16


def split2(v):
    high = v.astype(BF16)
    return high, (v - high.astype(F32)).astype(BF16)


def dot(a, b, contract=((1,), (0,))):
    return lax.dot_general(a, b, (contract, ((), ())), preferred_element_type=F32)


def layer(
    group, rows_y, nchan,
    x_hbm, gate_hbm, b_hbm, c_hbm, step_hbm, keep_hbm, skip_hbm, gain_hbm,
    base_s, total_ref,
    x_s, gate_s, b_s, c_s, keep_step, skip_s, gain_s,
    keep8, step8, coef8, cum8, c2_s,
    totals, device_total, block_state, starts, prefix_s,
    end_s, gather1, totals1, group_prefix, group_total_state, group_total,
    gather2, totals2, entering_s, decay_s, back_s, gather3,
    slope_s, squares_s, gather_sq, lines_s,
    load_sem, keep_sem, skip_sem, y_in, z_in,
    send_sem, b_recv, d_recv, e_recv, f_recv,
):
    tokens, channels = x_s.shape
    nstate = b_s.shape[0]
    heads = keep_step.shape[1]
    width = channels // heads
    blocks = tokens // BLOCK
    tiles = channels // LANES
    per_tile = heads // tiles
    piece = 2 * nstate // group

    me = lax.axis_index("seq")
    me_z = lax.axis_index("chan")
    me_y = me // group
    me_j = me % group
    is_owner = me_j % 2 == 1
    me_q = me_j // 2

    def owner(q):
        return 2 * q + 1

    def at_group(j):
        return (me_y * group + j, me_z)

    def at_y(y):
        return (y * group + me_j, me_z)

    def lines_of(count, semaphore):
        ref = lines_s.at[pl.ds(0, count)]
        return pltpu.make_async_remote_copy(
            ref, ref, semaphore, semaphore,
            device_id=(me, (me_z + 1) % nchan), device_id_type=MESH,
        )

    def arrived(count, semaphore):
        lines_of(count, semaphore).wait_recv()

    def sent(count):
        lines_of(count, send_sem).wait_send()

    owners = group // 2
    both_lines = nstate * tokens // (2 * channels) + tokens // 2

    def loaded(count, i):
        ref = lines_s.at[pl.ds(0, count)]
        pltpu.make_async_copy(ref, ref, load_sem.at[i]).wait()

    def rank(y):
        return jnp.minimum(y, rows_y - y) * rows_y + y

    by_rank = sorted(range(rows_y), key=lambda y: min(y, rows_y - y) * rows_y + y)

    first = [
        pltpu.make_async_copy(keep_hbm, keep_step.at[0], keep_sem),
        pltpu.make_async_copy(step_hbm, keep_step.at[1], keep_sem),
        pltpu.make_async_copy(b_hbm, b_s, load_sem.at[0]),
    ]
    parts = [
        pltpu.make_async_copy(x_hbm.at[part, :], x_s.at[part, :], load_sem.at[0])
        for part in (pl.ds(i * (tokens // 4), tokens // 4) for i in range(4))
    ]
    second = [
        pltpu.make_async_copy(c_hbm, c_s, load_sem.at[1]),
        pltpu.make_async_copy(gate_hbm, gate_s, load_sem.at[1]),
        pltpu.make_async_copy(gain_hbm, gain_s, load_sem.at[1]),
        pltpu.make_async_copy(skip_hbm, skip_s, skip_sem),
    ]
    for copy in first:
        copy.start()
    for copy in parts:
        copy.start(priority=1)

    barrier = pltpu.get_barrier_semaphore()

    def greet(device):
        pl.semaphore_signal(barrier, inc=1, device_id=device, device_id_type=MESH)

    def report(semaphore, device):
        pl.semaphore_signal(semaphore, inc=1, device_id=device, device_id_type=MESH)

    for j in range(group):

        @pl.when((j != me_j) & is_owner)
        def _():
            greet(at_group(j))

    for y in range(rows_y):

        @pl.when(is_owner & (rank(me_y) < rank(y)))
        def _():
            greet(at_y(y))

    for z in range(nchan):

        @pl.when(me_z < z)
        def _():
            greet((me, z))

    lane = lax.broadcasted_iota(jnp.int32, (8, channels), 1)
    row8 = lax.broadcasted_iota(jnp.int32, (8, channels), 0)
    own_head = (lane // width) == row8
    half = lax.broadcasted_iota(jnp.int32, (1, LANES), 1) < width
    past = lax.broadcasted_iota(jnp.int32, (BLOCK, BLOCK), 0)
    here = lax.broadcasted_iota(jnp.int32, (BLOCK, BLOCK), 1)
    upper = jnp.where(past <= here, 1.0, 0.0).astype(BF16)
    later = jnp.where(past > here, 1.0, 0.0).astype(BF16)

    pltpu.make_async_copy(keep_step, keep_step, keep_sem).wait()
    for copy in second:
        copy.start()
    keep8[...] = jnp.zeros_like(keep8)
    step8[...] = jnp.zeros_like(step8)
    for k in range(blocks):
        keep8[8 * k : 8 * k + heads, :] = keep_step[0, :, BLOCK * k : BLOCK * (k + 1)]
        step8[8 * k : 8 * k + heads, :] = keep_step[1, :, BLOCK * k : BLOCK * (k + 1)]
    keep = keep8[...]
    k_high = keep.astype(BF16)
    k_mid, k_low = split2(keep - k_high.astype(F32))
    after = dot(k_high, later) + (dot(k_mid, later) + dot(k_low, later))
    coef8[...] = jnp.exp(after) * step8[...]

    loaded(both_lines, 0)
    cum8[...] = dot(k_high, upper) + (dot(k_mid, upper) + dot(k_low, upper))
    for k in range(blocks):
        coef = coef8[8 * k : 8 * k + 8, :]
        bt = b_s[:, BLOCK * k : BLOCK * (k + 1)].astype(F32)
        for t in range(tiles):
            lines = jnp.concatenate(
                [(bt * coef[h : h + 1, :]).astype(BF16) for h in (2 * t, 2 * t + 1)], axis=0
            )
            both = dot(lines, x_s[BLOCK * k : BLOCK * (k + 1), LANES * t : LANES * (t + 1)])
            block_state[k, :, LANES * t : LANES * (t + 1)] = jnp.where(
                half, both[:nstate], both[nstate:]
            )
    for k in range(blocks):
        last = cum8[8 * k : 8 * k + 8, BLOCK - 1 : BLOCK]
        spread = jnp.where(own_head, jnp.broadcast_to(last, (8, channels)), 0.0)
        totals[k : k + 1, :] = jnp.sum(spread, axis=0, keepdims=True)
    device_total[...] = jnp.sum(totals[...], axis=0, keepdims=True)
    running = jnp.zeros((nstate, channels), F32)
    for k in range(blocks):
        starts[k] = running
        running = jnp.exp(totals[k : k + 1, :]) * running + block_state[k]
    for q in range(group // 2):
        end_s[q] = running[piece * q : piece * (q + 1), :]

    greeted = me_z + jnp.where(is_owner, owners - 1, owners)
    for y in range(rows_y):
        greeted = greeted + jnp.where(is_owner & (rank(y) < rank(me_y)), 1, 0)
    pl.semaphore_wait(barrier, greeted)

    for y in range(rows_y):

        @pl.when(is_owner & (y < me_y) & (rank(y) < rank(me_y)))
        def _():
            report(y_in.at[me_y], at_y(y))

    def copy_a(i):
        return pltpu.make_async_remote_copy(
            device_total, totals1.at[me_j], send_sem, b_recv,
            device_id=at_group(owner((me_q + i) % (group // 2))), device_id_type=MESH,
        )

    def copy_b(i):
        q = (me_q + i) % (group // 2)
        return pltpu.make_async_remote_copy(
            end_s.at[q], gather1.at[me_j], send_sem, b_recv,
            device_id=at_group(owner(q)), device_id_type=MESH,
        )

    others = [group // 4] + [i for i in range(group // 2) if i != group // 4]
    for i in others:

        @pl.when((i != 0) | jnp.logical_not(is_owner))
        def _():
            copy_a(i).start()
            copy_b(i).start()

    for z in range(nchan):

        @pl.when(z < me_z)
        def _():
            report(z_in, (me, z))

    @pl.when(is_owner)
    def _():
        gather1[me_j] = end_s[me_q]
        totals1[me_j] = device_total[...]

    before = jnp.zeros((1, channels), F32)
    for k in range(blocks):
        prefix_s[k : k + 1, :] = before
        before = before + totals[k : k + 1, :]

    loaded(both_lines + 1, 1)
    second[-1].wait()
    head_of = lax.broadcasted_iota(jnp.int32, (1, channels), 1) // width
    skip_row = jnp.zeros((1, channels), F32)
    for h in range(heads):
        skip_row = jnp.where(head_of == h, skip_s[0, h], skip_row)
    diagonal = (
        lax.broadcasted_iota(jnp.int32, (LANES, LANES), 0)
        >= lax.broadcasted_iota(jnp.int32, (LANES, LANES), 1)
    )

    def inside(k, carry):
        rows = pl.ds(pl.multiple_of(k * BLOCK, BLOCK), BLOCK)
        slab_at = pl.ds(pl.multiple_of(k * 8, 8), 8)
        slab = cum8[slab_at, :]
        steps = step8[slab_at, :]
        columns = jnp.transpose(slab)
        c_block = c_s[:, rows]
        c_pair = jnp.transpose(jnp.concatenate([c_block, c_block], axis=0))
        c2_s[rows, :] = c_pair
        scores = dot(c_pair[:, :nstate], b_s[:, rows])
        high, low = split2(starts[k])
        read = dot(c_pair, jnp.concatenate([high, low], axis=0))
        carried = jnp.exp(prefix_s[pl.ds(k, 1), :])
        for t in range(tiles):
            lanes = slice(LANES * t, LANES * (t + 1))
            weights, spreads = [], []
            for h in (2 * t, 2 * t + 1):
                column = jnp.broadcast_to(columns[:, h : h + 1], (BLOCK, LANES))
                spreads.append(column)

                def weight(r, s):
                    rr, ss = slice(LANES * r, LANES * (r + 1)), slice(LANES * s, LANES * (s + 1))
                    w = (
                        scores[rr, ss]
                        * jnp.exp(column[rr, :] - slab[h : h + 1, ss])
                        * steps[h : h + 1, ss]
                    )
                    return (jnp.where(diagonal, w, 0.0) if r == s else w).astype(BF16)

                top = jnp.concatenate([weight(0, 0), jnp.zeros((LANES, LANES), BF16)], axis=1)
                bottom = jnp.concatenate([weight(1, 0), weight(1, 1)], axis=1)
                weights += [top, bottom]
            x_tile = x_s[rows, lanes]
            both = dot(jnp.concatenate(weights, axis=0), x_tile)
            value = jnp.where(half, both[:BLOCK], both[BLOCK:])
            value = value + skip_row[:, lanes] * x_tile.astype(F32)
            gate = gate_s[rows, lanes].astype(F32)
            gate = gate / (1.0 + jnp.exp(-gate))
            slope = jnp.exp(jnp.where(half, spreads[0], spreads[1])) * gate
            base_s[rows, lanes] = value * gate + slope * read[:, lanes]
            slope_s[rows, lanes] = slope * carried[:, lanes]
        return carry

    third = (blocks * 3) // 8
    middle = jnp.where(me_y > 0, third + blocks // 4, third)
    lax.fori_loop(0, third, inside, 0)

    def copy_c(y):
        return pltpu.make_async_remote_copy(
            group_total, totals2.at[me_y], send_sem, d_recv,
            device_id=at_y(y), device_id_type=MESH,
        )

    def copy_d(y):
        return pltpu.make_async_remote_copy(
            group_total_state, gather2.at[me_y], send_sem, d_recv,
            device_id=at_y(y), device_id_type=MESH,
        )

    @pl.when(is_owner)
    def _():
        arrived((group - 1) * (piece + 1), b_recv)
        total = totals1[0]
        for m in range(1, group):
            total = total + totals1[m]
        group_total[...] = total
        state = jnp.zeros((piece, channels), F32)
        for m in range(group):
            group_prefix[m] = state
            state = jnp.exp(totals1[m]) * state + gather1[m]
        group_total_state[...] = state
        for y in by_rank:

            @pl.when((y > me_y) & (rank(me_y) < rank(y)))
            def _():
                pl.semaphore_wait(y_in.at[y], 1)

            @pl.when(y > me_y)
            def _():
                copy_c(y).start()
                copy_d(y).start()

    def copy_e(i):
        p = (me_j + i) % group
        return pltpu.make_async_remote_copy(
            back_s.at[p], gather3.at[me_q], send_sem, e_recv,
            device_id=at_group(p), device_id_type=MESH,
        )

    @pl.when(is_owner)
    def _():
        ahead = jnp.zeros((1, channels), F32)
        for m in range(group):
            decay_s[m] = jnp.exp(ahead)
            ahead = ahead + totals1[m]

    lax.fori_loop(third, middle, inside, 0)

    @pl.when(is_owner)
    def _():
        entering_s[...] = jnp.zeros_like(entering_s)
        for n in range(1, rows_y):

            @pl.when(me_y == n)
            def _():
                arrived(n * (piece + 1), d_recv)
                state = gather2[0]
                for y in range(1, n):
                    state = jnp.exp(totals2[y]) * state + gather2[y]
                entering_s[...] = state

        entering = entering_s[...]
        for i in sorted(range(1, group), key=lambda i: i % 2 - 2 * min((i + 1) // 2, (group - i) // 2) - 3 * (i % 2)):
            p = (me_j + i) % group
            back_s[p] = decay_s[p] * entering + group_prefix[p]
            copy_e(i).start()
        back_s[me_j] = decay_s[me_j] * entering + group_prefix[me_j]
        gather3[me_q] = back_s[me_j]

    lax.fori_loop(middle, blocks, inside, 0)

    @pl.when(is_owner)
    def _():
        arrived((owners - 1) * piece, e_recv)

    @pl.when(jnp.logical_not(is_owner))
    def _():
        arrived(owners * piece, e_recv)

    high, low = split2(jnp.concatenate([gather3[q] for q in range(group // 2)], axis=0))
    incoming = jnp.concatenate([high, low], axis=0)
    sums = jnp.zeros((BLOCK, LANES), F32)
    place = lax.broadcasted_iota(jnp.int32, (BLOCK, LANES), 1)
    for k in range(blocks):
        rows = slice(BLOCK * k, BLOCK * (k + 1))
        read = dot(c2_s[rows, :], incoming)
        gated = base_s[rows, :] + slope_s[rows, :] * read
        base_s[rows, :] = gated
        square = gated * gated
        partial = square[:, :LANES]
        for t in range(1, tiles):
            partial = partial + square[:, LANES * t : LANES * (t + 1)]
        sums = jnp.where(place == k, jnp.sum(partial, axis=1, keepdims=True), sums)
    squares_s[...] = jnp.transpose(sums)[:blocks, :]

    def copy_f(z):
        return pltpu.make_async_remote_copy(
            squares_s, gather_sq.at[me_z], send_sem, f_recv,
            device_id=(me, z), device_id_type=MESH,
        )

    for z in range(nchan):

        @pl.when(z < me_z)
        def _():
            copy_f(z).start()

    @pl.when(me_z < nchan - 1)
    def _():
        pl.semaphore_wait(z_in, nchan - 1 - me_z)

    for z in range(nchan):

        @pl.when(z > me_z)
        def _():
            copy_f(z).start()

    gather_sq[me_z] = squares_s[...]
    for k in range(blocks):
        rows = slice(BLOCK * k, BLOCK * (k + 1))
        base_s[rows, :] = base_s[rows, :] * gain_s[...]

    arrived((nchan - 1) * blocks, f_recv)

    total = gather_sq[0]
    for z in range(1, nchan):
        total = total + gather_sq[z]
    total_ref[...] = total

    for n in range(rows_y):

        @pl.when(is_owner & (me_y == rows_y - 1 - n))
        def _():
            sent((owners - 1 + n) * (piece + 1) + (group - 1) * piece + (nchan - 1) * blocks)

    @pl.when(jnp.logical_not(is_owner))
    def _():
        sent(owners * (piece + 1) + (nchan - 1) * blocks)


def scale_rows(width, base_ref, total_ref, out_hbm, out_s, store_sem):
    tokens, channels = base_ref.shape
    blocks = tokens // BLOCK
    factor = lax.rsqrt(total_ref[...] / width + EPSILON)
    for k in range(blocks):
        for r in range(BLOCK // LANES):
            part = slice(LANES * r, LANES * (r + 1))
            rows = slice(BLOCK * k + LANES * r, BLOCK * k + LANES * (r + 1))
            scale = jnp.transpose(jnp.broadcast_to(factor[k : k + 1, part], (LANES, LANES)))
            for t in range(channels // LANES):
                lanes = slice(LANES * t, LANES * (t + 1))
                out_s[rows, lanes] = (base_ref[rows, lanes] * scale).astype(BF16)
        rows = slice(BLOCK * k, BLOCK * (k + 1))
        pltpu.make_async_copy(out_s.at[rows, :], out_hbm.at[rows, :], store_sem).start()
    pltpu.make_async_copy(out_s, out_hbm, store_sem).wait()


def per_device(group, rows_y, nchan, x, gate, b, c, step, keep, skip, gain):
    tokens, channels = x.shape
    nstate = b.shape[1]
    heads = step.shape[0]
    blocks = tokens // BLOCK
    owners = group // 2
    piece = nstate // owners
    vmem = pltpu.VMEM
    dma = pltpu.SemaphoreType.DMA
    anywhere = pl.BlockSpec(memory_space=pl.ANY)
    operands = (x, gate, b.T, c.T, step, keep, skip.reshape(1, heads), gain.reshape(1, channels))
    scratch = [
        vmem((tokens, channels), BF16), vmem((tokens, channels), BF16),
        vmem((nstate, tokens), BF16), vmem((nstate, tokens), BF16),
        vmem((2, heads, tokens), F32),
        pltpu.SMEM((1, heads), F32), vmem((1, channels), F32),
        vmem((8 * blocks, BLOCK), F32), vmem((8 * blocks, BLOCK), F32),
        vmem((8 * blocks, BLOCK), F32), vmem((8 * blocks, BLOCK), F32),
        vmem((tokens, 2 * nstate), BF16),
        vmem((blocks, channels), F32), vmem((1, channels), F32),
        vmem((blocks, nstate, channels), F32), vmem((blocks, nstate, channels), F32),
        vmem((blocks, channels), F32),
        vmem((owners, piece, channels), F32), vmem((group, piece, channels), F32),
        vmem((group, 1, channels), F32), vmem((group, piece, channels), F32),
        vmem((piece, channels), F32), vmem((1, channels), F32),
        vmem((rows_y, piece, channels), F32), vmem((rows_y, 1, channels), F32),
        vmem((piece, channels), F32), vmem((group, 1, channels), F32),
        vmem((group, piece, channels), F32), vmem((owners, piece, channels), F32),
        vmem((tokens, channels), F32),
        vmem((blocks, BLOCK), F32), vmem((nchan, blocks, BLOCK), F32),
        vmem((max((owners + rows_y) * (piece + 1) + group * piece + nchan * blocks, nstate * tokens // (2 * channels) + tokens // 2 + 1), 1, channels), F32),
        dma((2,)), dma, dma, pltpu.SemaphoreType.REGULAR((rows_y,)), pltpu.SemaphoreType.REGULAR,
    ] + [dma] * 5
    base, total = pl.pallas_call(
        functools.partial(layer, group, rows_y, nchan),
        out_shape=(
            jax.ShapeDtypeStruct((tokens, channels), F32),
            jax.ShapeDtypeStruct((blocks, BLOCK), F32),
        ),
        in_specs=[anywhere] * 8,
        out_specs=(pl.BlockSpec(memory_space=pltpu.VMEM),) * 2,
        scratch_shapes=scratch,
        compiler_params=pltpu.CompilerParams(
            collective_id=0, has_side_effects=True, vmem_limit_bytes=24 * 1024 * 1024
        ),
    )(*[pltpu.with_memory_space_constraint(v, pltpu.HBM) for v in operands])
    return pl.pallas_call(
        functools.partial(scale_rows, channels * nchan),
        out_shape=jax.ShapeDtypeStruct((tokens, channels), BF16),
        in_specs=[pl.BlockSpec(memory_space=pltpu.VMEM)] * 2,
        out_specs=anywhere,
        scratch_shapes=[vmem((tokens, channels), BF16), dma],
        compiler_params=pltpu.CompilerParams(vmem_limit_bytes=8 * 1024 * 1024),
    )(base, total)


def build(mesh, group):
    rows_y = mesh.shape["seq"] // group
    placed = (
        P("seq", "chan"), P("seq", "chan"), P("seq", None), P("seq", None),
        P("chan", "seq"), P("chan", "seq"), P("chan"), P("chan"),
    )
    return jax.shard_map(
        functools.partial(per_device, group, rows_y, mesh.shape["chan"]),
        mesh=mesh, in_specs=placed, out_specs=P("seq", "chan"), check_vma=False,
    )


def solution(mesh):
    return build(mesh, GROUP)
```
